8 devices in a mesh: dp: 1 (over z), ep: 2 (over y), tp: 4 (over x, core).
Axes of the slice: x: 2, y: 2, z: 1, core: 2. Of those that a mesh axis runs over, the one named last changes fastest.
Arguments:
- X: bfloat16 [256, 2048], P(('dp', 'ep', 'tp'))
- idx: int32 [256, 8], P(('dp', 'ep', 'tp'))
- g: float32 [256, 8], P(('dp', 'ep', 'tp'))
- W1: bfloat16 [64, 2048, 1024], P('ep', None, 'tp')
- W3: bfloat16 [64, 2048, 1024], P('ep', None, 'tp')
- W2: bfloat16 [64, 1024, 2048], P('ep', 'tp')
Outputs:
- output: bfloat16 [256, 2048], P(('dp', 'ep', 'tp'))
All inputs are finite; a program needn't handle non-finite values.
Results may differ from the reference program's by a relative error of at most 0.0101844.
Values are sent between devices in bfloat16 or wider.
A program may use at most 1 GiB of HBM per device.

```python
import jax
import jax.numpy as jnp
from jax import lax

D = 2048
F = 1024
E = 64
TOP = 8
T_LOC = 32
NDEV = 8
C = 2 * TOP * T_LOC // E
T = NDEV * T_LOC


def _weights(key, shape, fan):
    def one(k):
        return (jax.random.normal(k, shape, jnp.float32) * fan ** -0.5).astype(jnp.bfloat16)
    return lax.map(one, jax.random.split(key, E))


def setup_inputs(seed: int = 0, part: int = 0) -> dict:
    key = jax.random.PRNGKey(seed)
    kdata, kw = jax.random.split(key)
    kx, kr, kg = jax.random.split(jax.random.fold_in(kdata, part), 3)
    k1, k3, k2 = jax.random.split(kw, 3)
    x = jax.random.normal(kx, (T, D), jnp.float32).astype(jnp.bfloat16)
    expert_rank = jnp.arange(E, dtype=jnp.uint32)
    wait_scale = jnp.uint32(512) - (jnp.uint32(256) * expert_rank) // jnp.uint32(max(E - 1, 1))
    wait_time = (jax.random.bits(jax.random.fold_in(kr, 7), (T, E), jnp.uint32) >> 10) * wait_scale[None, :]
    idx = jnp.argsort(wait_time, axis=1)[:, :TOP].astype(jnp.int32)
    g = jax.random.uniform(kg, (T, TOP), jnp.float32, 0.25, 1.0)
    return {"X": x, "idx": idx, "g": g,
            "W1": _weights(k1, (D, F), D), "W3": _weights(k3, (D, F), D), "W2": _weights(k2, (F, D), F)}


def _slots(ids):
    oh = (ids[:, None] == jnp.arange(E, dtype=jnp.int32)[None, :]).astype(jnp.int32)
    return jnp.sum(oh * (jnp.cumsum(oh, axis=0) - 1), axis=1)


def reference(X, idx, g, W1, W3, W2):
    ids = idx.reshape(NDEV, T_LOC * TOP)
    s = jax.vmap(_slots)(ids)
    keep = s < C
    dest = jnp.where(keep, ids * C + s, E * C)
    xr = jnp.repeat(X.reshape(NDEV, T_LOC, D), TOP, axis=1)
    buf = jax.vmap(lambda x, dd: jnp.zeros((E * C, D), X.dtype).at[dd].set(x, mode="drop"))(xr, dest)
    buf = buf.reshape(NDEV, E, C, D).transpose(1, 0, 2, 3)

    def expert(a):
        xb, w1, w3, w2 = a

        def rows(x):
            h1 = jnp.dot(x, w1, preferred_element_type=jnp.float32)
            h3 = jnp.dot(x, w3, preferred_element_type=jnp.float32)
            h = (jax.nn.silu(h1) * h3).astype(jnp.bfloat16)
            return jnp.dot(h, w2, preferred_element_type=jnp.float32).astype(jnp.bfloat16)
        return lax.map(rows, xb)

    yb = lax.map(expert, (buf, W1, W3, W2))
    yb = yb.transpose(1, 0, 2, 3).reshape(NDEV, E * C, D)
    ysel = jax.vmap(lambda y, dd: y[jnp.minimum(dd, E * C - 1)])(yb, dest)
    wgt = jnp.where(keep, g.reshape(NDEV, T_LOC * TOP), 0.0)
    out = jnp.sum(ysel.astype(jnp.float32).reshape(NDEV, T_LOC, TOP, D) * wgt.reshape(NDEV, T_LOC, TOP, 1), axis=2)
    return out.reshape(T, D).astype(jnp.bfloat16)
```

```python
import functools

import jax
import jax.numpy as jnp
from jax import lax
from jax.experimental import pallas as pl
from jax.experimental.pallas import tpu as pltpu
from jax.sharding import PartitionSpec as P

CF = 2
NS = 20
CW = 512
GE = 8
F32, BF16 = jnp.float32, jnp.bfloat16


def _dot(a, b):
    return jnp.dot(a, b, preferred_element_type=F32)


def _kernel(n_el, cap, x_ref, idx_ref, g_ref, w1_ref, w3_ref, w2_ref, o_ref,
            xall, idxv, gv, gall, xg, ring, hbuf, gt, pt, ybuf, yacc, yrecv, ssum, rfin,
            in_sem, wsem, xs_sem, xr_sem, xf_sem, xp_sem, gs_sem, gr_sem, gf_sem, gp_sem,
            ys_sem, yr_sem, zs_sem, zr_sem):
    ep, tp = lax.axis_index("ep"), lax.axis_index("tp")
    dp = lax.axis_index("dp")
    core = lax.rem(tp, 2)
    chip = ep * 2 + tp // 2
    t_loc, d = x_ref.shape
    top = idx_ref.shape[1]
    n_exp = 2 * n_el
    n_chunk = d // CW
    n_grp = n_el // GE
    n_item = n_el + n_chunk * n_grp
    kt, kd = w1_ref.shape[1], w1_ref.shape[2]
    fl = w1_ref.shape[3]

    def dev(r, flip):
        e2 = 1 - ep if r & 2 else ep
        x2 = 1 - tp // 2 if r & 1 else tp // 2
        c2 = 1 - core if flip else core
        return (dp, e2, x2 * 2 + c2)

    def chip_of(r):
        e2 = 1 - ep if r & 2 else ep
        x2 = 1 - tp // 2 if r & 1 else tp // 2
        return e2 * 2 + x2

    def remote(src, dst, ss, rs, to):
        return pltpu.make_async_remote_copy(src_ref=src, dst_ref=dst, send_sem=ss, recv_sem=rs, device_id=to,
                                            device_id_type=pl.DeviceIdType.MESH)

    def w13_copies(e, slot):
        return (pltpu.make_async_copy(w1_ref.at[e], ring.at[slot, :, :, pl.ds(0, fl)], wsem.at[slot, 0]),
                pltpu.make_async_copy(w3_ref.at[e], ring.at[slot, :, :, pl.ds(fl, fl)], wsem.at[slot, 1]))

    def w2_copies(b, slot):
        c, q = b // n_grp, b % n_grp
        half = GE // 2
        col = pl.multiple_of(c * CW, CW)
        return tuple(
            pltpu.make_async_copy(w2_ref.at[pl.ds(q * GE + s * half, half), :, pl.ds(col, CW)],
                                  ring.at[slot, pl.ds(s * half, half)], wsem.at[slot, s])
            for s in range(2))

    def start_item(i):
        slot = lax.rem(i, NS)

        @pl.when(i < n_el)
        def _():
            for c in w13_copies(i, slot):
                c.start()

        @pl.when(jnp.logical_and(i >= n_el, i < n_item))
        def _():
            for c in w2_copies(i - n_el, slot):
                c.start()

    mine = xall.at[chip, pl.ds(core * t_loc, t_loc)]
    x_in = pltpu.make_async_copy(x_ref, mine, in_sem.at[0])
    i_in = pltpu.make_async_copy(idx_ref, idxv, in_sem.at[1])
    g_in = pltpu.make_async_copy(g_ref, gv, in_sem.at[2])
    x_in.start()
    i_in.start()
    g_in.start()
    barrier = pltpu.get_barrier_semaphore()
    peers = [(1, False), (2, False), (3, False), (0, True)]
    for r, flip in peers:
        pl.semaphore_signal(barrier, inc=1, device_id=dev(r, flip), device_id_type=pl.DeviceIdType.MESH)

    def prime(i, _):
        start_item(i)
        return 0

    lax.fori_loop(0, NS, prime, 0)
    x_in.wait()
    i_in.wait()
    g_in.wait()
    pl.semaphore_wait(barrier, len(peers))

    def x_copy(r, flip):
        return remote(mine, mine, xs_sem.at[r], xp_sem.at[0] if flip else xr_sem.at[r], dev(r, flip))

    for r in (3, 1, 2):
        x_copy(r, False).start()
    x_copy(0, True).start()

    ids, gates = idxv[...], gv[...]
    lane = lax.broadcasted_iota(jnp.int32, (t_loc, 2 * n_exp), 1)
    e_of = lax.rem(lane, n_exp)
    gd = jnp.zeros((t_loc, 2 * n_exp), F32)
    hit = jnp.zeros((t_loc, 2 * n_exp), F32)
    for j in range(top):
        eq = ids[:, j:j + 1] == e_of
        gd = jnp.where(eq, gates[:, j:j + 1], gd)
        hit = jnp.where(eq, 1.0, hit)
    before = (lax.broadcasted_iota(jnp.int32, (t_loc, t_loc), 1)
              < lax.broadcasted_iota(jnp.int32, (t_loc, t_loc), 0)).astype(BF16)
    slot = _dot(before, hit.astype(BF16))
    keep = jnp.logical_and(hit > 0.5, slot < cap - 0.5)
    gall[chip, pl.ds(core * t_loc, t_loc)] = jnp.where(keep, jnp.where(lane < n_exp, gd, slot),
                                                       jnp.where(lane < n_exp, 0.0, -1.0))
    gmine = gall.at[chip, pl.ds(core * t_loc, t_loc)]

    def g_copy(r, flip):
        return remote(gmine, gmine, gs_sem.at[r], gp_sem.at[0] if flip else gr_sem.at[r], dev(r, flip))

    for r in (3, 1, 2):
        g_copy(r, False).start()
    g_copy(0, True).start()

    def fwd(buf, ss, ps, r):
        ref = buf.at[chip_of(r), pl.ds(core * t_loc, t_loc)]
        return remote(ref, ref, ss.at[r], ps.at[r], dev(0, True))

    def arrived(buf, ps, r):
        ref = buf.at[chip_of(r), pl.ds((1 - core) * t_loc, t_loc)]
        return remote(ref, ref, xs_sem.at[0], ps.at[r], dev(0, True))

    def landed(buf, rs, r):
        ref = buf.at[chip_of(r), pl.ds(core * t_loc, t_loc)]
        return remote(ref, ref, xs_sem.at[0], rs.at[r], dev(r, False))

    pair = 2 * t_loc
    nk = n_el * 2 * cap
    el = lax.broadcasted_iota(jnp.int32, (2 * n_exp, nk), 1) // (2 * cap) + ep * n_el
    row = lax.broadcasted_iota(jnp.int32, (2 * n_exp, nk), 0)
    ex_g = (row == el).astype(BF16)
    ex_s = (row == el + n_exp).astype(BF16)
    kl = lax.broadcasted_iota(jnp.int32, (pair, nk), 1)
    tr = lax.broadcasted_iota(jnp.int32, (pair, nk), 0)
    same_core = lax.rem(kl // cap, 2) == tr // t_loc
    s_of = lax.rem(kl, cap).astype(F32)

    def dispatch(r):
        q = chip_of(r)
        gs = gall[q]
        hi = gs.astype(BF16)
        r1 = gs - hi.astype(F32)
        mid = r1.astype(BF16)
        lo = (r1 - mid.astype(F32)).astype(BF16)
        here = jnp.logical_and(_dot(hi, ex_s) == s_of, same_core)
        for k, part in enumerate((hi, mid, lo)):
            gt[q, pl.ds(k * pair, pair)] = jnp.where(here, _dot(part, ex_g), 0.0).astype(BF16)
        pt[...] = jnp.where(here, 1.0, 0.0).T.astype(BF16)
        for c in range(d // CW):
            rows = _dot(pt[...], xall[q, :, c * CW:(c + 1) * CW])
            xg[:, q, :, c * CW:(c + 1) * CW] = rows.astype(BF16).reshape(n_el, 2 * cap, CW)

    for r in (0, 1, 2, 3):
        if r:
            landed(xall, xr_sem, r).wait_recv()
            fwd(xall, xf_sem, xp_sem, r).start()
            landed(gall, gr_sem, r).wait_recv()
            fwd(gall, gf_sem, gp_sem, r).start()
    for r in (0, 1, 2, 3):
        arrived(xall, xp_sem, r).wait_recv()
        arrived(gall, gp_sem, r).wait_recv()
        dispatch(r)

    m = 8 * cap

    def wait13(e):
        for c in w13_copies(e, lax.rem(e, NS)):
            c.wait()

    def up(k, _):
        e0 = 2 * k
        wait13(e0)
        wait13(e0 + 1)
        acc = []
        for j in range(2):
            w = ring[lax.rem(e0 + j, NS)].reshape(kt * kd, 2 * fl)
            acc.append(_dot(xg[e0 + j].reshape(m, d), w))
        for j in range(2):
            a, b = acc[j][:, :fl], acc[j][:, fl:]
            hbuf[e0 + j] = (a * jax.nn.sigmoid(a) * b).astype(BF16)
        start_item(e0 + NS)
        start_item(e0 + 1 + NS)
        return 0

    lax.fori_loop(0, n_el // 2, up, 0)

    def y_copy(c):
        return remote(yacc.at[c, 1 - core], yrecv.at[c], ys_sem.at[c], yr_sem.at[c], dev(0, True))

    def z_copy(c, r):
        return remote(ssum.at[c, chip_of(r)], rfin.at[c, chip], zs_sem.at[c, r], zr_sem.at[c, r], dev(r, False))

    def z_landed(c, r):
        return remote(ssum.at[c, chip_of(r)], rfin.at[c, chip_of(r)], zs_sem.at[c, r], zr_sem.at[c, r], dev(r, False))

    def second(c):
        y_copy(c).wait_recv()
        ssum[c] = yacc[c, core] + yrecv[c]
        for r in (3, 1, 2):
            z_copy(c, r).start()

    def down(b, _):
        c, q = b // n_grp, b % n_grp
        slot = lax.rem(b + n_el, NS)
        for cp in w2_copies(b, slot):
            cp.wait()
        for j in range(GE):
            y = _dot(hbuf[q * GE + j], ring[slot, j])
            ybuf[q * GE + j] = y.astype(BF16).reshape(4, 2 * cap, CW)
        start_item(b + n_el + NS)

        @pl.when(jnp.logical_and(q == 1, c > 0))
        def _():
            second(c - 1)

        @pl.when(q == n_grp - 1)
        def _():
            for p in range(4):
                z = _dot(gt[p], ybuf[:, p].reshape(nk, CW))
                z = z[:pair] + z[pair:2 * pair] + z[2 * pair:]
                for k in range(2):
                    yacc[c, k, p] = z[k * t_loc:(k + 1) * t_loc]
            y_copy(c).start()

        return 0

    lax.fori_loop(0, n_chunk * n_grp, down, 0)
    second(n_chunk - 1)
    for c in range(n_chunk):
        tot = ssum[c, chip]
        for r in (1, 2, 3):
            z_landed(c, r).wait_recv()
            tot = tot + rfin[c, chip_of(r)]
        o_ref[:, c * CW:(c + 1) * CW] = tot

    for r in (3, 1, 2):
        x_copy(r, False).wait_send()
        g_copy(r, False).wait_send()
        fwd(xall, xf_sem, xp_sem, r).wait_send()
        fwd(gall, gf_sem, gp_sem, r).wait_send()
    x_copy(0, True).wait_send()
    g_copy(0, True).wait_send()
    for c in range(n_chunk):
        y_copy(c).wait_send()
        for r in (1, 2, 3):
            z_copy(c, r).wait_send()


def solution(mesh):
    rows = P(("dp", "ep", "tp"), None)

    def local(x, idx, g, w1, w3, w2):
        t_loc, d = x.shape
        top = idx.shape[1]
        el, _, fl = w1.shape
        n_exp = 2 * el
        cap = CF * top * t_loc // n_exp
        nc = d // CW
        nk = el * 2 * cap
        dma, vm = pltpu.SemaphoreType.DMA, pltpu.VMEM
        any_ = pl.BlockSpec(memory_space=pl.ANY)
        y = pl.pallas_call(
            functools.partial(_kernel, el, cap),
            out_shape=jax.ShapeDtypeStruct((t_loc, d), F32),
            in_specs=[any_] * 6,
            out_specs=pl.BlockSpec(memory_space=pltpu.VMEM),
            scratch_shapes=[
                vm((4, 2 * t_loc, d), BF16),
                vm((t_loc, top), jnp.int32),
                vm((t_loc, top), F32),
                vm((4, 2 * t_loc, 2 * n_exp), F32),
                vm((el, 4, 2 * cap, d), BF16),
                vm((NS, d // fl, fl, 2 * fl), BF16),
                vm((el, 8 * cap, fl), BF16),
                vm((4, 6 * t_loc, nk), BF16),
                vm((nk, 2 * t_loc), BF16),
                vm((el, 4, 2 * cap, CW), BF16),
                vm((nc, 2, 4, t_loc, CW), F32),
                vm((nc, 4, t_loc, CW), F32),
                vm((nc, 4, t_loc, CW), F32),
                vm((nc, 4, t_loc, CW), F32),
                dma((3,)), dma((NS, 2)),
                dma((4,)), dma((4,)), dma((4,)), dma((4,)),
                dma((4,)), dma((4,)), dma((4,)), dma((4,)),
                dma((nc,)), dma((nc,)), dma((nc, 4)), dma((nc, 4)),
            ],
            compiler_params=pltpu.CompilerParams(collective_id=0, has_side_effects=True,
                                                 vmem_limit_bytes=67043328),
            name="moe",
        )(x, idx, g, w1.reshape(el, d // fl, fl, fl), w3.reshape(el, d // fl, fl, fl), w2)
        return y.astype(BF16)

    return jax.shard_map(local, mesh=mesh,
                         in_specs=(rows, rows, rows, P("ep", None, "tp"), P("ep", None, "tp"), P("ep", "tp", None)),
                         out_specs=rows, check_vma=False)
```

```python
import functools

import jax
import jax.numpy as jnp
from jax import lax
from jax.experimental import pallas as pl
from jax.experimental.pallas import tpu as pltpu
from jax.sharding import PartitionSpec as P

CF = 2
NS = 20
PRIME = (4, 12, 16, 18, NS)
CW = 512
GE = 8
F32, BF16 = jnp.float32, jnp.bfloat16


def _dot(a, b):
    return jnp.dot(a, b, preferred_element_type=F32)


def _kernel(n_el, cap, x_ref, idx_ref, g_ref, w1_ref, w3_ref, w2_ref, o_ref,
            xall, idxv, gv, gall, xg, ring, hbuf, gt, pt, ybuf, yacc, yrecv, ssum, rfin,
            in_sem, wsem, xs_sem, xr_sem, xf_sem, xp_sem, gs_sem, gr_sem, gf_sem, gp_sem,
            ys_sem, yr_sem, zs_sem, zr_sem):
    ep, tp = lax.axis_index("ep"), lax.axis_index("tp")
    dp = lax.axis_index("dp")
    core = lax.rem(tp, 2)
    chip = ep * 2 + tp // 2
    t_loc, d = x_ref.shape
    top = idx_ref.shape[0]
    n_exp = 2 * n_el
    n_chunk = d // CW
    n_grp = n_el // GE
    n_item = n_el + n_chunk * n_grp
    kt, kd = w1_ref.shape[1], w1_ref.shape[2]
    fl = w1_ref.shape[3]

    def dev(r, flip):
        e2 = 1 - ep if r & 2 else ep
        x2 = 1 - tp // 2 if r & 1 else tp // 2
        c2 = 1 - core if flip else core
        return (dp, e2, x2 * 2 + c2)

    def chip_of(r):
        e2 = 1 - ep if r & 2 else ep
        x2 = 1 - tp // 2 if r & 1 else tp // 2
        return e2 * 2 + x2

    def remote(src, dst, ss, rs, to):
        return pltpu.make_async_remote_copy(src_ref=src, dst_ref=dst, send_sem=ss, recv_sem=rs, device_id=to,
                                            device_id_type=pl.DeviceIdType.MESH)

    def w13_copies(e, slot):
        return (pltpu.make_async_copy(w1_ref.at[e], ring.at[slot, :, :, pl.ds(0, fl)], wsem.at[slot, 0]),
                pltpu.make_async_copy(w3_ref.at[e], ring.at[slot, :, :, pl.ds(fl, fl)], wsem.at[slot, 1]))

    def w2_copies(b, slot):
        c, q = b // n_grp, b % n_grp
        half = GE // 2
        col = pl.multiple_of(c * CW, CW)
        return tuple(
            pltpu.make_async_copy(w2_ref.at[pl.ds(q * GE + s * half, half), :, pl.ds(col, CW)],
                                  ring.at[slot, pl.ds(s * half, half)], wsem.at[slot, s])
            for s in range(2))

    def start_item(i):
        slot = lax.rem(i, NS)

        @pl.when(i < n_el)
        def _():
            for c in w13_copies(i, slot):
                c.start()

        @pl.when(jnp.logical_and(i >= n_el, i < n_item))
        def _():
            for c in w2_copies(i - n_el, slot):
                c.start()

    mine = xall.at[chip, pl.ds(core * t_loc, t_loc)]
    x_in = pltpu.make_async_copy(x_ref, mine, in_sem.at[0])
    i_in = pltpu.make_async_copy(idx_ref, idxv, in_sem.at[1])
    g_in = pltpu.make_async_copy(g_ref, gv, in_sem.at[2])
    x_in.start()
    i_in.start()
    g_in.start()
    barrier = pltpu.get_barrier_semaphore()
    peers = [(1, False), (2, False), (3, False), (0, True)]
    for r, flip in peers:
        pl.semaphore_signal(barrier, inc=1, device_id=dev(r, flip), device_id_type=pl.DeviceIdType.MESH)

    def prime(i, _):
        start_item(i)
        return 0

    lax.fori_loop(0, PRIME[0], prime, 0)
    x_in.wait()
    i_in.wait()
    g_in.wait()
    pl.semaphore_wait(barrier, len(peers))

    def x_copy(r, flip):
        return remote(mine, mine, xs_sem.at[r], xp_sem.at[0] if flip else xr_sem.at[r], dev(r, flip))

    for r in (3, 1, 2):
        x_copy(r, False).start()
    x_copy(0, True).start()

    ids, gates = idxv[...], gv[...]
    line = lax.broadcasted_iota(jnp.int32, (2 * n_exp, t_loc), 0)
    e_of = lax.rem(line, n_exp)
    gd = jnp.zeros((2 * n_exp, t_loc), F32)
    hit = jnp.zeros((2 * n_exp, t_loc), F32)
    for j in range(top):
        eq = ids[j:j + 1] == e_of
        gd = jnp.where(eq, gates[j:j + 1], gd)
        hit = jnp.where(eq, 1.0, hit)
    before = (lax.broadcasted_iota(jnp.int32, (t_loc, t_loc), 0)
              < lax.broadcasted_iota(jnp.int32, (t_loc, t_loc), 1)).astype(BF16)
    slot = _dot(hit.astype(BF16), before)
    keep = jnp.logical_and(hit > 0.5, slot < cap - 0.5)
    table = jnp.where(keep, jnp.where(line < n_exp, gd, slot), jnp.where(line < n_exp, 0.0, -1.0))
    gall[chip, pl.ds(core * t_loc, t_loc)] = table.T
    lax.fori_loop(PRIME[0], PRIME[1], prime, 0)
    gmine = gall.at[chip, pl.ds(core * t_loc, t_loc)]

    def g_copy(r, flip):
        return remote(gmine, gmine, gs_sem.at[r], gp_sem.at[0] if flip else gr_sem.at[r], dev(r, flip))

    for r in (3, 1, 2):
        g_copy(r, False).start()
    g_copy(0, True).start()

    def fwd(buf, ss, ps, r):
        ref = buf.at[chip_of(r), pl.ds(core * t_loc, t_loc)]
        return remote(ref, ref, ss.at[r], ps.at[r], dev(0, True))

    def arrived(buf, ps, r):
        ref = buf.at[chip_of(r), pl.ds((1 - core) * t_loc, t_loc)]
        return remote(ref, ref, xs_sem.at[0], ps.at[r], dev(0, True))

    def landed(buf, rs, r):
        ref = buf.at[chip_of(r), pl.ds(core * t_loc, t_loc)]
        return remote(ref, ref, xs_sem.at[0], rs.at[r], dev(r, False))

    pair = 2 * t_loc
    nk = n_el * 2 * cap
    el = lax.broadcasted_iota(jnp.int32, (2 * n_exp, nk), 1) // (2 * cap) + ep * n_el
    row = lax.broadcasted_iota(jnp.int32, (2 * n_exp, nk), 0)
    ex_g = (row == el).astype(BF16)
    ex_s = (row == el + n_exp).astype(BF16)
    kl = lax.broadcasted_iota(jnp.int32, (pair, nk), 1)
    tr = lax.broadcasted_iota(jnp.int32, (pair, nk), 0)
    same_core = lax.rem(kl // cap, 2) == tr // t_loc
    s_of = lax.rem(kl, cap).astype(F32)

    def dispatch(r):
        q = chip_of(r)
        gs = gall[q]
        hi = gs.astype(BF16)
        r1 = gs - hi.astype(F32)
        mid = r1.astype(BF16)
        lo = (r1 - mid.astype(F32)).astype(BF16)
        here = jnp.logical_and(_dot(hi, ex_s) == s_of, same_core)
        for k, part in enumerate((hi, mid, lo)):
            gt[q, pl.ds(k * pair, pair)] = jnp.where(here, _dot(part, ex_g), 0.0).astype(BF16)
        pt[...] = jnp.where(here, 1.0, 0.0).T.astype(BF16)
        for c in range(d // CW):
            rows = _dot(pt[...], xall[q, :, c * CW:(c + 1) * CW])
            xg[:, q, :, c * CW:(c + 1) * CW] = rows.astype(BF16).reshape(n_el, 2 * cap, CW)

    def settle(r):
        arrived(xall, xp_sem, r).wait_recv()
        arrived(gall, gp_sem, r).wait_recv()
        dispatch(r)

    settle(0)
    for k, r in enumerate((2, 3, 1)):
        landed(xall, xr_sem, r).wait_recv()
        fwd(xall, xf_sem, xp_sem, r).start()
        landed(gall, gr_sem, r).wait_recv()
        fwd(gall, gf_sem, gp_sem, r).start()
        lax.fori_loop(PRIME[k + 1], PRIME[k + 2], prime, 0)
    for r in (2, 3, 1):
        settle(r)

    m = 8 * cap

    def wait13(e):
        for c in w13_copies(e, lax.rem(e, NS)):
            c.wait()

    def up(k, _):
        e0 = 2 * k
        wait13(e0)
        wait13(e0 + 1)
        acc = []
        for j in range(2):
            w = ring[lax.rem(e0 + j, NS)].reshape(kt * kd, 2 * fl)
            acc.append(_dot(xg[e0 + j].reshape(m, d), w))
        for j in range(2):
            a, b = acc[j][:, :fl], acc[j][:, fl:]
            hbuf[e0 + j] = (a * jax.nn.sigmoid(a) * b).astype(BF16)
        start_item(e0 + NS)
        start_item(e0 + 1 + NS)
        return 0

    lax.fori_loop(0, n_el // 2, up, 0)

    def y_copy(c):
        return remote(yacc.at[c, 1 - core], yrecv.at[c], ys_sem.at[c], yr_sem.at[c], dev(0, True))

    def z_copy(c, r):
        return remote(ssum.at[c, chip_of(r)], rfin.at[c, chip], zs_sem.at[c, r], zr_sem.at[c, r], dev(r, False))

    def z_landed(c, r):
        return remote(ssum.at[c, chip_of(r)], rfin.at[c, chip_of(r)], zs_sem.at[c, r], zr_sem.at[c, r], dev(r, False))

    def second(c):
        y_copy(c).wait_recv()
        ssum[c] = yacc[c, core] + yrecv[c]
        for r in (3, 1, 2):
            z_copy(c, r).start()

    def down(b, _):
        c, q = b // n_grp, b % n_grp
        slot = lax.rem(b + n_el, NS)
        for cp in w2_copies(b, slot):
            cp.wait()
        for j in range(GE):
            y = _dot(hbuf[q * GE + j], ring[slot, j])
            ybuf[q * GE + j] = y.astype(BF16).reshape(4, 2 * cap, CW)
        start_item(b + n_el + NS)

        @pl.when(jnp.logical_and(q == 1, c > 0))
        def _():
            second(c - 1)

        @pl.when(q == n_grp - 1)
        def _():
            for p in range(4):
                z = _dot(gt[p], ybuf[:, p].reshape(nk, CW))
                z = z[:pair] + z[pair:2 * pair] + z[2 * pair:]
                for k in range(2):
                    yacc[c, k, p] = z[k * t_loc:(k + 1) * t_loc]
            y_copy(c).start()

        return 0

    lax.fori_loop(0, n_chunk * n_grp, down, 0)
    second(n_chunk - 1)
    for c in range(n_chunk):
        tot = ssum[c, chip]
        for r in (1, 2, 3):
            z_landed(c, r).wait_recv()
            tot = tot + rfin[c, chip_of(r)]
        o_ref[:, c * CW:(c + 1) * CW] = tot

    for r in (3, 1, 2):
        x_copy(r, False).wait_send()
        g_copy(r, False).wait_send()
        fwd(xall, xf_sem, xp_sem, r).wait_send()
        fwd(gall, gf_sem, gp_sem, r).wait_send()
    x_copy(0, True).wait_send()
    g_copy(0, True).wait_send()
    for c in range(n_chunk):
        y_copy(c).wait_send()
        for r in (1, 2, 3):
            z_copy(c, r).wait_send()


def solution(mesh):
    rows = P(("dp", "ep", "tp"), None)

    def local(x, idx, g, w1, w3, w2):
        t_loc, d = x.shape
        top = idx.shape[1]
        el, _, fl = w1.shape
        n_exp = 2 * el
        cap = CF * top * t_loc // n_exp
        nc = d // CW
        nk = el * 2 * cap
        dma, vm = pltpu.SemaphoreType.DMA, pltpu.VMEM
        any_ = pl.BlockSpec(memory_space=pl.ANY)
        y = pl.pallas_call(
            functools.partial(_kernel, el, cap),
            out_shape=jax.ShapeDtypeStruct((t_loc, d), F32),
            in_specs=[any_] * 6,
            out_specs=pl.BlockSpec(memory_space=pltpu.VMEM),
            scratch_shapes=[
                vm((4, 2 * t_loc, d), BF16),
                vm((top, t_loc), jnp.int32),
                vm((top, t_loc), F32),
                vm((4, 2 * t_loc, 2 * n_exp), F32),
                vm((el, 4, 2 * cap, d), BF16),
                vm((NS, d // fl, fl, 2 * fl), BF16),
                vm((el, 8 * cap, fl), BF16),
                vm((4, 6 * t_loc, nk), BF16),
                vm((nk, 2 * t_loc), BF16),
                vm((el, 4, 2 * cap, CW), BF16),
                vm((nc, 2, 4, t_loc, CW), F32),
                vm((nc, 4, t_loc, CW), F32),
                vm((nc, 4, t_loc, CW), F32),
                vm((nc, 4, t_loc, CW), F32),
                dma((3,)), dma((NS, 2)),
                dma((4,)), dma((4,)), dma((4,)), dma((4,)),
                dma((4,)), dma((4,)), dma((4,)), dma((4,)),
                dma((nc,)), dma((nc,)), dma((nc, 4)), dma((nc, 4)),
            ],
            compiler_params=pltpu.CompilerParams(collective_id=0, has_side_effects=True,
                                                 vmem_limit_bytes=67043328),
            name="moe",
        )(x, idx.T, g.T, w1.reshape(el, d // fl, fl, fl), w3.reshape(el, d // fl, fl, fl), w2)
        return y.astype(BF16)

    return jax.shard_map(local, mesh=mesh,
                         in_specs=(rows, rows, rows, P("ep", None, "tp"), P("ep", None, "tp"), P("ep", "tp", None)),
                         out_specs=rows, check_vma=False)
```

```python
import functools

import jax
import jax.numpy as jnp
from jax import lax
from jax.experimental import pallas as pl
from jax.experimental.pallas import tpu as pltpu
from jax.sharding import PartitionSpec as P

CF = 2
NS = 20
PRIME = (4, 12, NS)
KW = 512
NW = 8
UP = 4
CW = 256
GE = 16
F32, BF16 = jnp.float32, jnp.bfloat16


def _dot(a, b):
    return jnp.dot(a, b, preferred_element_type=F32)


def _kernel(n_el, cap, x_ref, idx_ref, g_ref, w1_ref, w3_ref, w2_ref, o_ref,
            xall, idxv, gv, sall, gall, xg, ring, acc, hbuf, gt, pt, ybuf, yacc, yrecv, ssum, rfin,
            in_sem, wsem, xs_sem, xr_sem, xf_sem, xp_sem, ss_sem, sr_sem, sf_sem, sp_sem, gs_sem, gr_sem, gf_sem, gp_sem,
            ys_sem, yr_sem, zs_sem, zr_sem):
    ep, tp = lax.axis_index("ep"), lax.axis_index("tp")
    dp = lax.axis_index("dp")
    core = lax.rem(tp, 2)
    chip = ep * 2 + tp // 2
    t_loc, d = x_ref.shape
    top = idx_ref.shape[0]
    n_exp = 2 * n_el
    n_chunk = d // CW
    n_grp = n_el // GE
    n_item = n_el + n_chunk * n_grp
    kt, kd = w1_ref.shape[1], w1_ref.shape[2]
    fl = w1_ref.shape[3]
    n_k = d // KW
    rows = pl.ds(core * t_loc, t_loc)
    other = pl.ds((1 - core) * t_loc, t_loc)

    def dev(r, flip):
        e2 = 1 - ep if r & 2 else ep
        x2 = 1 - tp // 2 if r & 1 else tp // 2
        c2 = 1 - core if flip else core
        return (dp, e2, x2 * 2 + c2)

    def chip_of(r):
        e2 = 1 - ep if r & 2 else ep
        x2 = 1 - tp // 2 if r & 1 else tp // 2
        return e2 * 2 + x2

    def remote(src, dst, ss, rs, to):
        return pltpu.make_async_remote_copy(src_ref=src, dst_ref=dst, send_sem=ss, recv_sem=rs, device_id=to,
                                            device_id_type=pl.DeviceIdType.MESH)

    def w13_copies(e, slot):
        return (pltpu.make_async_copy(w1_ref.at[e], ring.at[slot, :, :, pl.ds(0, fl)], wsem.at[slot, 0]),
                pltpu.make_async_copy(w3_ref.at[e], ring.at[slot, :, :, pl.ds(fl, fl)], wsem.at[slot, 1]))

    def w2_copies(b, slot):
        c, q = b // n_grp, b % n_grp
        half = GE // 2
        col = pl.multiple_of(c * CW, CW)
        return tuple(
            pltpu.make_async_copy(w2_ref.at[pl.ds(q * GE + s * half, half), :, pl.ds(col, CW)],
                                  ring.at[slot, :, :, pl.ds(s * CW, CW)], wsem.at[slot, s])
            for s in range(2))

    def start_item(i):
        slot = lax.rem(i, NS)

        @pl.when(i < n_el)
        def _():
            for c in w13_copies(i, slot):
                c.start()

        @pl.when(jnp.logical_and(i >= n_el, i < n_item))
        def _():
            for c in w2_copies(i - n_el, slot):
                c.start()

    def prime(i, _):
        start_item(i)
        return 0

    x_in = [pltpu.make_async_copy(x_ref.at[:, pl.ds(k * KW, KW)], xall.at[k, chip, rows], in_sem.at[2 + k])
            for k in range(n_k)]
    i_in = pltpu.make_async_copy(idx_ref, idxv, in_sem.at[0])
    g_in = pltpu.make_async_copy(g_ref, gv, in_sem.at[1])
    i_in.start()
    g_in.start()
    for c in x_in:
        c.start()
    barrier = pltpu.get_barrier_semaphore()
    peers = [(1, False), (2, False), (3, False), (0, True)]
    for r, flip in peers:
        pl.semaphore_signal(barrier, inc=1, device_id=dev(r, flip), device_id_type=pl.DeviceIdType.MESH)
    lax.fori_loop(0, PRIME[0], prime, 0)
    i_in.wait()
    g_in.wait()

    ids, gates = idxv[...], gv[...]
    line = lax.broadcasted_iota(jnp.int32, (2 * n_exp, t_loc), 0)
    gd = jnp.zeros((2 * n_exp, t_loc), F32)
    hit = jnp.zeros((2 * n_exp, t_loc), F32)
    for j in range(top):
        eq = ids[j:j + 1] == line
        gd = jnp.where(eq, gates[j:j + 1], gd)
        hit = jnp.where(eq, 1.0, hit)
    before = (lax.broadcasted_iota(jnp.int32, (t_loc, t_loc), 0)
              < lax.broadcasted_iota(jnp.int32, (t_loc, t_loc), 1)).astype(BF16)
    slot = _dot(hit.astype(BF16), before)
    keep = jnp.logical_and(hit > 0.5, slot < cap - 0.5)
    sall[chip, rows] = jnp.where(keep, slot, -1.0).T.astype(BF16)
    gall[chip, rows] = jnp.where(keep, gd, 0.0).T

    for c in x_in:
        c.wait()
    pl.semaphore_wait(barrier, len(peers))

    class Gather:
        def __init__(self, buf, ss, rs, fs, ps):
            self.buf, self.ss, self.rs, self.fs, self.ps = buf, ss, rs, fs, ps

        def out(self, r):
            ref = self.buf.at[chip, rows]
            return remote(ref, ref, self.ss.at[r], self.rs.at[r] if r else self.ps.at[0], dev(r, r == 0))

        def landed(self, r):
            ref = self.buf.at[chip_of(r), rows]
            return remote(ref, ref, self.ss.at[r], self.rs.at[r], dev(r, False))

        def fwd(self, r):
            ref = self.buf.at[chip_of(r), rows]
            return remote(ref, ref, self.fs.at[r], self.ps.at[r], dev(0, True))

        def arrived(self, r):
            ref = self.buf.at[chip_of(r), other]
            return remote(ref, ref, self.fs.at[r], self.ps.at[r], dev(0, True))

        def send(self):
            for r in (3, 1, 2, 0):
                self.out(r).start()

        def forward(self):
            for r in (2, 3, 1):
                self.landed(r).wait_recv()
                self.fwd(r).start()

        def settle(self):
            for r in (0, 2, 3, 1):
                self.arrived(r).wait_recv()

        def drain(self):
            for r in (3, 1, 2):
                self.out(r).wait_send()
                self.fwd(r).wait_send()
            self.out(0).wait_send()

    xs = [Gather(xall.at[k], xs_sem.at[k], xr_sem.at[k], xf_sem.at[k], xp_sem.at[k]) for k in range(n_k)]
    sg = Gather(sall, ss_sem, sr_sem, sf_sem, sp_sem)
    gg = Gather(gall, gs_sem, gr_sem, gf_sem, gp_sem)
    sg.send()
    for x in xs:
        x.send()
    gg.send()
    lax.fori_loop(PRIME[0], PRIME[1], prime, 0)

    pair = 2 * t_loc
    nk = n_el * 2 * cap
    m = 8 * cap
    el = lax.broadcasted_iota(jnp.int32, (2 * n_exp, nk), 1) // (2 * cap) + ep * n_el
    expand = (lax.broadcasted_iota(jnp.int32, (2 * n_exp, nk), 0) == el).astype(BF16)
    kl = lax.broadcasted_iota(jnp.int32, (pair, nk), 1)
    tr = lax.broadcasted_iota(jnp.int32, (pair, nk), 0)
    want = jnp.where(lax.rem(kl // cap, 2) == tr // t_loc, lax.rem(kl, cap), -2).astype(F32)

    sg.forward()
    sg.settle()
    for q in range(4):
        pt[q] = jnp.where(_dot(sall[q], expand) == want, 1.0, 0.0).T.astype(BF16)
    lax.fori_loop(PRIME[1], PRIME[2], prime, 0)

    def wait13(e):
        for c in w13_copies(e, lax.rem(e, NS)):
            c.wait()

    def swiglu(v):
        a, b = v[:, :fl], v[:, fl:]
        return (a * jax.nn.sigmoid(a) * b).astype(BF16)

    xs[0].forward()
    for k in range(n_k):
        xs[k].settle()
        for q in range(4):
            got = _dot(pt[q], xall[k, q])
            xg[k, :, q] = got.astype(BF16).reshape(n_el, 2 * cap, KW)
        if k + 1 < n_k:
            xs[k + 1].forward()
        else:
            gg.forward()

        def part(u, _, k=k):
            for j in range(UP):
                e = u * UP + j
                if k == 0:
                    wait13(e)
            vals = []
            for j in range(UP):
                e = u * UP + j
                w = ring[lax.rem(e, NS), k * (KW // kd):(k + 1) * (KW // kd)].reshape(KW, 2 * fl)
                vals.append(_dot(xg[k, e].reshape(m, KW), w))
            for j in range(UP):
                e = u * UP + j
                v = vals[j] if k == 0 else acc[e] + vals[j]
                if k + 1 < n_k:
                    acc[e] = v
                else:
                    hbuf[e] = swiglu(v)
            if k + 1 == n_k:
                for j in range(UP):
                    start_item(u * UP + j + NS)
            return 0

        lax.fori_loop(0, NW // UP, part, 0)

    gg.settle()
    for q in range(4):
        here = _dot(sall[q], expand) == want
        gs = gall[q]
        hi = gs.astype(BF16)
        r1 = gs - hi.astype(F32)
        mid = r1.astype(BF16)
        lo = (r1 - mid.astype(F32)).astype(BF16)
        for k, p in enumerate((hi, mid, lo)):
            gt[q, pl.ds(k * pair, pair)] = jnp.where(here, _dot(p, expand), 0.0).astype(BF16)

    def up(u, _):
        for j in range(UP):
            wait13(u * UP + j)
        vals = []
        for j in range(UP):
            e = u * UP + j
            w = ring[lax.rem(e, NS)].reshape(n_k, KW, 2 * fl)
            v = _dot(xg[0, e].reshape(m, KW), w[0])
            for k in range(1, n_k):
                v = v + _dot(xg[k, e].reshape(m, KW), w[k])
            vals.append(v)
        for j in range(UP):
            hbuf[u * UP + j] = swiglu(vals[j])
        for j in range(UP):
            start_item(u * UP + j + NS)
        return 0

    lax.fori_loop(NW // UP, n_el // UP, up, 0)

    def y_copy(c):
        return remote(yacc.at[c, 1 - core], yrecv.at[c], ys_sem.at[c], yr_sem.at[c], dev(0, True))

    def z_copy(c, r):
        return remote(ssum.at[c, chip_of(r)], rfin.at[c, chip], zs_sem.at[c, r], zr_sem.at[c, r], dev(r, False))

    def z_landed(c, r):
        return remote(ssum.at[c, chip_of(r)], rfin.at[c, chip_of(r)], zs_sem.at[c, r], zr_sem.at[c, r], dev(r, False))

    def second(c):
        y_copy(c).wait_recv()
        ssum[c] = yacc[c, core] + yrecv[c]
        for r in (3, 1, 2):
            z_copy(c, r).start()

    def down(b, _):
        c, q = b // n_grp, b % n_grp
        slot = lax.rem(b + n_el, NS)
        for cp in w2_copies(b, slot):
            cp.wait()
        for j in range(GE):
            half = GE // 2
            w = ring[slot, j % half, :, (j // half) * CW:(j // half + 1) * CW]
            ybuf[q * GE + j] = _dot(hbuf[q * GE + j], w).astype(BF16).reshape(4, 2 * cap, CW)
        start_item(b + n_el + NS)

        @pl.when(jnp.logical_and(q == 0, c > 0))
        def _():
            second(c - 1)

        @pl.when(q == n_grp - 1)
        def _():
            for p in range(4):
                z = _dot(gt[p], ybuf[:, p].reshape(nk, CW))
                z = z[:pair] + z[pair:2 * pair] + z[2 * pair:]
                for k in range(2):
                    yacc[c, k, p] = z[k * t_loc:(k + 1) * t_loc]
            y_copy(c).start()

        return 0

    lax.fori_loop(0, n_chunk * n_grp, down, 0)
    second(n_chunk - 1)
    for c in range(n_chunk):
        tot = ssum[c, chip]
        for r in (1, 2, 3):
            z_landed(c, r).wait_recv()
            tot = tot + rfin[c, chip_of(r)]
        o_ref[:, c * CW:(c + 1) * CW] = tot

    for x in xs + [sg, gg]:
        x.drain()
    for c in range(n_chunk):
        y_copy(c).wait_send()
        for r in (1, 2, 3):
            z_copy(c, r).wait_send()


def solution(mesh):
    rows = P(("dp", "ep", "tp"), None)

    def local(x, idx, g, w1, w3, w2):
        t_loc, d = x.shape
        top = idx.shape[1]
        el, _, fl = w1.shape
        n_exp = 2 * el
        cap = CF * top * t_loc // n_exp
        nc = d // CW
        nk = el * 2 * cap
        dma, vm = pltpu.SemaphoreType.DMA, pltpu.VMEM
        any_ = pl.BlockSpec(memory_space=pl.ANY)
        y = pl.pallas_call(
            functools.partial(_kernel, el, cap),
            out_shape=jax.ShapeDtypeStruct((t_loc, d), F32),
            in_specs=[any_] * 6,
            out_specs=pl.BlockSpec(memory_space=pltpu.VMEM),
            scratch_shapes=[
                vm((d // KW, 4, 2 * t_loc, KW), BF16),
                vm((top, t_loc), jnp.int32),
                vm((top, t_loc), F32),
                vm((4, 2 * t_loc, 2 * n_exp), BF16),
                vm((4, 2 * t_loc, 2 * n_exp), F32),
                vm((d // KW, el, 4, 2 * cap, KW), BF16),
                vm((NS, d // fl, fl, 2 * fl), BF16),
                vm((NW, 8 * cap, 2 * fl), F32),
                vm((el, 8 * cap, fl), BF16),
                vm((4, 6 * t_loc, nk), BF16),
                vm((4, nk, 2 * t_loc), BF16),
                vm((el, 4, 2 * cap, CW), BF16),
                vm((nc, 2, 4, t_loc, CW), F32),
                vm((nc, 4, t_loc, CW), F32),
                vm((nc, 4, t_loc, CW), F32),
                vm((nc, 4, t_loc, CW), F32),
                dma((2 + d // KW,)), dma((NS, 2)),
                *[dma((d // KW, 4))] * 4, *[dma((4,))] * 8,
                dma((nc,)), dma((nc,)), dma((nc, 4)), dma((nc, 4)),
            ],
            compiler_params=pltpu.CompilerParams(collective_id=0, has_side_effects=True,
                                                 vmem_limit_bytes=67043328),
            name="moe",
        )(x, idx.T, g.T, w1.reshape(el, d // fl, fl, fl), w3.reshape(el, d // fl, fl, fl), w2)
        return y.astype(BF16)

    return jax.shard_map(local, mesh=mesh,
                         in_specs=(rows, rows, rows, P("ep", None, "tp"), P("ep", None, "tp"), P("ep", "tp", None)),
                         out_specs=rows, check_vma=False)
```

```python
import functools

import jax
import jax.numpy as jnp
from jax import lax
from jax.experimental import pallas as pl
from jax.experimental.pallas import tpu as pltpu
from jax.sharding import PartitionSpec as P

CF = 2
NP = 10
PRIME = (2, 6, NP)
KW = 512
NW = 8
UP = 8
CW = 256
F32, BF16 = jnp.float32, jnp.bfloat16


def _dot(a, b):
    return jnp.dot(a, b, preferred_element_type=F32)


def _kernel(n_el, cap, x_ref, idx_ref, g_ref, w1_ref, w3_ref, w2_ref, o_ref,
            xall, idxv, gv, sall, gall, xg, ring, acc, hbuf, gt, pt, ybuf, yacc, yrecv, ssum, rfin,
            in_sem, wsem, x_sem, xr_sem, xp_sem, s_sem, sr_sem, sp_sem, g_sem, gr_sem, gp_sem, y_sem, yr_sem, z_sem, zr_sem):
    ep, tp = lax.axis_index("ep"), lax.axis_index("tp")
    dp = lax.axis_index("dp")
    core = lax.rem(tp, 2)
    chip = ep * 2 + tp // 2
    t_loc, d = x_ref.shape
    top = idx_ref.shape[0]
    n_exp = 2 * n_el
    n_chunk = d // CW
    kd, fl = w1_ref.shape[2], w1_ref.shape[3]
    n_k = d // KW
    n_w13 = n_el // 2
    n_pair = n_w13 + n_chunk
    rows = pl.ds(core * t_loc, t_loc)
    other = pl.ds((1 - core) * t_loc, t_loc)

    def dev(r, flip):
        e2 = 1 - ep if r & 2 else ep
        x2 = 1 - tp // 2 if r & 1 else tp // 2
        c2 = 1 - core if flip else core
        return (dp, e2, x2 * 2 + c2)

    def chip_of(r):
        e2 = 1 - ep if r & 2 else ep
        x2 = 1 - tp // 2 if r & 1 else tp // 2
        return e2 * 2 + x2

    def remote(src, dst, ss, rs, to):
        return pltpu.make_async_remote_copy(src_ref=src, dst_ref=dst, send_sem=ss, recv_sem=rs, device_id=to,
                                            device_id_type=pl.DeviceIdType.MESH)

    def wait_bytes(ref, sem):
        pltpu.make_async_copy(ref, ref, sem).wait()

    def start(p):
        slot = lax.rem(p, NP)
        left, right = pl.ds(0, fl), pl.ds(fl, fl)

        @pl.when(p < n_w13)
        def _():
            for w, half in ((w1_ref, left), (w3_ref, right)):
                pltpu.make_async_copy(w.at[pl.ds(2 * p, 2)], ring.at[slot, :, :, :, half], wsem.at[slot]).start()

        @pl.when(jnp.logical_and(p >= n_w13, p < n_pair))
        def _():
            cols = pl.ds(pl.multiple_of((p - n_w13) * CW, CW), CW)
            for k, half in enumerate((left, right)):
                pltpu.make_async_copy(w2_ref.at[pl.ds(2 * k, 2), :, :, cols], ring.at[slot, :, :, :, half],
                                      wsem.at[slot]).start()

    def wait(p):
        slot = lax.rem(p, NP)
        wait_bytes(ring.at[slot], wsem.at[slot])

    def prime(p, _):
        start(p)
        return 0

    x_in = [pltpu.make_async_copy(x_ref.at[:, pl.ds(k * KW, KW)], xall.at[k, chip, rows], in_sem.at[2 + k])
            for k in range(n_k)]
    i_in = pltpu.make_async_copy(idx_ref, idxv, in_sem.at[0])
    g_in = pltpu.make_async_copy(g_ref, gv, in_sem.at[1])
    i_in.start()
    g_in.start()
    for c in x_in:
        c.start()
    barrier = pltpu.get_barrier_semaphore()
    peers = [(1, False), (2, False), (3, False), (0, True)]
    for r, flip in peers:
        pl.semaphore_signal(barrier, inc=1, device_id=dev(r, flip), device_id_type=pl.DeviceIdType.MESH)
    lax.fori_loop(0, PRIME[0], prime, 0)
    i_in.wait()
    g_in.wait()

    ids, gates = idxv[...], gv[...]
    line = lax.broadcasted_iota(jnp.int32, (2 * n_exp, t_loc), 0)
    gd = jnp.zeros((2 * n_exp, t_loc), F32)
    hit = jnp.zeros((2 * n_exp, t_loc), F32)
    for j in range(top):
        eq = ids[j:j + 1] == line
        gd = jnp.where(eq, gates[j:j + 1], gd)
        hit = jnp.where(eq, 1.0, hit)
    before = (lax.broadcasted_iota(jnp.int32, (t_loc, t_loc), 0)
              < lax.broadcasted_iota(jnp.int32, (t_loc, t_loc), 1)).astype(BF16)
    slot = _dot(hit.astype(BF16), before)
    keep = jnp.logical_and(hit > 0.5, slot < cap - 0.5)
    sall[chip, rows] = jnp.where(keep, slot, -1.0).T.astype(BF16)
    gall[chip, rows] = jnp.where(keep, gd, 0.0).T

    for c in x_in:
        c.wait()
    pl.semaphore_wait(barrier, len(peers))

    def block(buf, r, k, mine=True):
        at = buf if k is None else buf.at[k]
        return at.at[chip_of(r), rows if mine else other]

    def send(buf, ss, rs, ps, k, to=(3, 1, 2, 0)):
        for r in to:
            ref = block(buf, 0, k)
            remote(ref, ref, ss, rs.at[r] if r else ps.at[0], dev(r, r == 0)).start()

    def forward(buf, ss, rs, ps, k):
        for r in (2, 3, 1):
            ref = block(buf, r, k)
            remote(ref, ref, ss, rs.at[r], dev(r, False)).wait_recv()
            remote(ref, ref, ss, ps.at[r], dev(0, True)).start()

    def settle(buf, ss, ps, k, froms):
        for r in froms:
            ref = block(buf, r, k, False)
            remote(ref, ref, ss, ps.at[r], dev(0, True)).wait_recv()

    sg = (sall, s_sem.at[0], sr_sem, sp_sem, None)
    gg = (gall, g_sem.at[0], gr_sem, gp_sem, None)
    xs = [(xall, x_sem.at[0], xr_sem.at[k], xp_sem.at[k], k) for k in range(n_k)]
    send(*sg)
    for x in xs:
        send(*x)
    send(*gg)
    lax.fori_loop(PRIME[0], PRIME[1], prime, 0)

    pair = 2 * t_loc
    nk = n_el * 2 * cap
    m = 8 * cap
    el = lax.broadcasted_iota(jnp.int32, (2 * n_exp, nk), 1) // (2 * cap) + ep * n_el
    expand = (lax.broadcasted_iota(jnp.int32, (2 * n_exp, nk), 0) == el).astype(BF16)
    kl = lax.broadcasted_iota(jnp.int32, (pair, nk), 1)
    tr = lax.broadcasted_iota(jnp.int32, (pair, nk), 0)
    want = jnp.where(lax.rem(kl // cap, 2) == tr // t_loc, lax.rem(kl, cap), -2).astype(F32)

    def plan(r):
        q = chip_of(r)
        pt[q] = jnp.where(_dot(sall[q], expand) == want, 1.0, 0.0).T.astype(BF16)

    def dispatch(k, r):
        q = chip_of(r)
        got = _dot(pt[q], xall[k, q])
        xg[k, :, q] = got.astype(BF16).reshape(n_el, 2 * cap, KW)

    settle(sall, s_sem.at[0], sp_sem, None, (0,))
    for x in xs:
        settle(xall, x_sem.at[0], x[3], x[4], (0,))
    plan(0)
    for k in range(n_k):
        dispatch(k, 0)
    forward(*sg)
    settle(sall, s_sem.at[0], sp_sem, None, (2, 3, 1))
    for r in (2, 3, 1):
        plan(r)
    lax.fori_loop(PRIME[1], PRIME[2], prime, 0)

    def swiglu(v):
        a, b = v[:, :fl], v[:, fl:]
        return (a * jax.nn.sigmoid(a) * b).astype(BF16)

    forward(*xs[0])
    for k in range(n_k):
        settle(xall, x_sem.at[0], xs[k][3], k, (2, 3, 1))
        if k + 1 < n_k:
            forward(*xs[k + 1])
        else:
            forward(*gg)
        if k == 0:
            for p in range(NW // 2):
                wait(p)
        for r in (2, 3, 1):
            dispatch(k, r)
        nt = KW // kd
        for e in range(NW):
            w = ring[e // 2, e % 2, k * nt:(k + 1) * nt].reshape(KW, 2 * fl)
            v = _dot(xg[k, e].reshape(m, KW), w)
            v = v if k == 0 else acc[e] + v
            if k + 1 < n_k:
                acc[e] = v
            else:
                hbuf[e] = swiglu(v)
    for p in range(NW // 2):
        start(p + NP)

    settle(gall, g_sem.at[0], gp_sem, None, (0, 2, 3, 1))
    here = (_dot(sall[...].reshape(4 * pair, 2 * n_exp), expand).reshape(4, pair, nk) == want)
    gs = gall[...].reshape(4 * pair, 2 * n_exp)
    hi = gs.astype(BF16)
    r1 = gs - hi.astype(F32)
    mid = r1.astype(BF16)
    lo = (r1 - mid.astype(F32)).astype(BF16)
    for k, p in enumerate((hi, mid, lo)):
        gt[:, pl.ds(k * pair, pair)] = jnp.where(here, _dot(p, expand).reshape(4, pair, nk), 0.0).astype(BF16)

    def up(u, _):
        for j in range(UP // 2):
            wait(u * (UP // 2) + j)
        for j in range(UP):
            e = u * UP + j
            w = ring[lax.rem(u * (UP // 2) + j // 2, NP), j % 2].reshape(n_k, KW, 2 * fl)
            v = _dot(xg[0, e].reshape(m, KW), w[0])
            for k in range(1, n_k):
                v = v + _dot(xg[k, e].reshape(m, KW), w[k])
            hbuf[e] = swiglu(v)
        for j in range(UP // 2):
            start(u * (UP // 2) + j + NP)
        return 0

    lax.fori_loop(NW // UP, n_el // UP, up, 0)

    wait_bytes(xall.at[pl.ds(0, n_k - 1)], x_sem.at[0])
    wait_bytes(xall.at[0, pl.ds(0, n_k // 2)], x_sem.at[0])
    for buf, sem in ((sall, s_sem), (gall, g_sem)):
        wait_bytes(buf.at[pl.ds(0, 3)], sem.at[0])
        wait_bytes(buf.at[0, pl.ds(0, t_loc)], sem.at[0])

    def y_copy(c):
        return remote(yacc.at[c, 1 - core], yrecv.at[c], y_sem.at[0], yr_sem.at[c], dev(0, True))

    def second(c):
        y_copy(c).wait_recv()
        ssum[c] = yacc[c, core] + yrecv[c]
        for r in (3, 1, 2):
            remote(ssum.at[c, chip_of(r)], rfin.at[c, r - 1], z_sem.at[0], zr_sem.at[c], dev(r, False)).start()

    def products(c):
        for e in range(n_el):
            i, j = e // 8, e % 8
            w = ring[lax.rem(c + n_w13, NP), i % 2, j, :, (i // 2) * CW:(i // 2 + 1) * CW]
            ybuf[lax.rem(c, 2), e] = _dot(hbuf[e], w).astype(BF16).reshape(4, 2 * cap, CW)

    def combine(c):
        for p in range(4):
            z = _dot(gt[p], ybuf[lax.rem(c, 2), :, p].reshape(nk, CW))
            z = z[:pair] + z[pair:2 * pair] + z[2 * pair:]
            for k in range(2):
                yacc[c, k, p] = z[k * t_loc:(k + 1) * t_loc]

    wait(n_w13)
    products(0)

    def down(c, _):
        wait(n_w13 + c)
        combine(c - 1)
        products(c)
        y_copy(c - 1).start()

        @pl.when(c > 1)
        def _():
            second(c - 2)

        return 0

    lax.fori_loop(1, n_chunk, down, 0)
    combine(n_chunk - 1)
    second(n_chunk - 2)
    y_copy(n_chunk - 1).start()

    def total(c):
        wait_bytes(rfin.at[c], zr_sem.at[c])
        o_ref[:, pl.ds(pl.multiple_of(c * CW, CW), CW)] = ssum[c, chip] + rfin[c, 0] + rfin[c, 1] + rfin[c, 2]

    for c in range(n_chunk - 4):
        total(c)
    second(n_chunk - 1)
    for c in range(n_chunk - 4, n_chunk):
        total(c)
    wait_bytes(yrecv, y_sem.at[0])
    wait_bytes(rfin, z_sem.at[0])


def solution(mesh):
    rows = P(("dp", "ep", "tp"), None)

    def local(x, idx, g, w1, w3, w2):
        t_loc, d = x.shape
        top = idx.shape[1]
        el, _, fl = w1.shape
        n_exp = 2 * el
        cap = CF * top * t_loc // n_exp
        nc = d // CW
        nk = el * 2 * cap
        dma, vm = pltpu.SemaphoreType.DMA, pltpu.VMEM
        any_ = pl.BlockSpec(memory_space=pl.ANY)
        y = pl.pallas_call(
            functools.partial(_kernel, el, cap),
            out_shape=jax.ShapeDtypeStruct((t_loc, d), F32),
            in_specs=[any_] * 6,
            out_specs=pl.BlockSpec(memory_space=pltpu.VMEM),
            scratch_shapes=[
                vm((d // KW, 4, 2 * t_loc, KW), BF16),
                vm((top, t_loc), jnp.int32),
                vm((top, t_loc), F32),
                vm((4, 2 * t_loc, 2 * n_exp), BF16),
                vm((4, 2 * t_loc, 2 * n_exp), F32),
                vm((d // KW, el, 4, 2 * cap, KW), BF16),
                vm((NP, 2, d // fl, fl, 2 * fl), BF16),
                vm((NW, 8 * cap, 2 * fl), F32),
                vm((el, 8 * cap, fl), BF16),
                vm((4, 6 * t_loc, nk), BF16),
                vm((4, nk, 2 * t_loc), BF16),
                vm((2, el, 4, 2 * cap, CW), BF16),
                vm((nc, 2, 4, t_loc, CW), F32),
                vm((nc, 4, t_loc, CW), F32),
                vm((nc, 4, t_loc, CW), F32),
                vm((nc, 3, t_loc, CW), F32),
                dma((2 + d // KW,)), dma((NP,)),
                dma((1,)), dma((d // KW, 4)), dma((d // KW, 4)),
                dma((1,)), dma((4,)), dma((4,)),
                dma((1,)), dma((4,)), dma((4,)),
                dma((1,)), dma((nc,)), dma((1,)), dma((nc,)),
            ],
            compiler_params=pltpu.CompilerParams(collective_id=0, has_side_effects=True,
                                                 vmem_limit_bytes=67043328),
            name="moe",
        )(x, idx.T, g.T, w1.reshape(el, d // fl, fl, fl), w3.reshape(el, d // fl, fl, fl),
          w2.reshape(el // 8, 8, fl, d))
        return y.astype(BF16)

    return jax.shard_map(local, mesh=mesh,
                         in_specs=(rows, rows, rows, P("ep", None, "tp"), P("ep", None, "tp"), P("ep", "tp", None)),
                         out_specs=rows, check_vma=False)
```

```python
import functools

import jax
import jax.numpy as jnp
from jax import lax
from jax.experimental import pallas as pl
from jax.experimental.pallas import tpu as pltpu
from jax.sharding import PartitionSpec as P

CF = 2
NP = 10
PRIME = (3, 4, 5, 6)
KW = 512
NW = 8
UP = 4
CW = 256
F32, BF16 = jnp.float32, jnp.bfloat16


def _dot(a, b):
    return jnp.dot(a, b, preferred_element_type=F32)


def _kernel(n_el, cap, x_ref, idx_ref, g_ref, w1_ref, w3_ref, w2_ref, o_ref,
            xall, idxv, gv, sall, gall, xg, ring, acc, hbuf, gt, pt, ybuf, yacc, yrecv, ssum, rfin,
            in_sem, wsem, x_sem, xr_sem, xp_sem, s_sem, sr_sem, sp_sem, g_sem, gr_sem, gp_sem, y_sem, yr_sem, z_sem, zr_sem):
    ep, tp = lax.axis_index("ep"), lax.axis_index("tp")
    dp = lax.axis_index("dp")
    core = lax.rem(tp, 2)
    chip = ep * 2 + tp // 2
    t_loc, d = x_ref.shape
    top = idx_ref.shape[0]
    n_exp = 2 * n_el
    n_chunk = d // CW
    kd, fl = w1_ref.shape[2], w1_ref.shape[3]
    n_k = d // KW
    n_w13 = n_el // 2
    n_pair = n_w13 + n_chunk
    rows = pl.ds(core * t_loc, t_loc)
    other = pl.ds((1 - core) * t_loc, t_loc)

    def dev(r, flip):
        e2 = 1 - ep if r & 2 else ep
        x2 = 1 - tp // 2 if r & 1 else tp // 2
        c2 = 1 - core if flip else core
        return (dp, e2, x2 * 2 + c2)

    def chip_of(r):
        e2 = 1 - ep if r & 2 else ep
        x2 = 1 - tp // 2 if r & 1 else tp // 2
        return e2 * 2 + x2

    def remote(src, dst, ss, rs, to):
        return pltpu.make_async_remote_copy(src_ref=src, dst_ref=dst, send_sem=ss, recv_sem=rs, device_id=to,
                                            device_id_type=pl.DeviceIdType.MESH)

    def wait_bytes(ref, sem):
        pltpu.make_async_copy(ref, ref, sem).wait()

    def start(p):
        slot = lax.rem(p, NP)
        left, right = pl.ds(0, fl), pl.ds(fl, fl)

        @pl.when(p < n_w13)
        def _():
            for i in range(2):
                for w, half in ((w1_ref, left), (w3_ref, right)):
                    for h in range(2):
                        part = pl.ds(h * 4, 4)
                        pltpu.make_async_copy(w.at[2 * p + i, part], ring.at[slot, i, part, :, half],
                                              wsem.at[slot]).start()

        @pl.when(jnp.logical_and(p >= n_w13, p < n_pair))
        def _():
            cols = pl.ds(pl.multiple_of((p - n_w13) * CW, CW), CW)
            for i in range(2):
                for k, half in enumerate((left, right)):
                    for h in range(2):
                        part = pl.ds(h * 4, 4)
                        pltpu.make_async_copy(w2_ref.at[2 * k + i, part, :, cols], ring.at[slot, i, part, :, half],
                                              wsem.at[slot]).start()

    def wait(p):
        slot = lax.rem(p, NP)
        wait_bytes(ring.at[slot], wsem.at[slot])

    def prime(p, _):
        start(p)
        return 0

    x_in = [pltpu.make_async_copy(x_ref.at[:, pl.ds(k * KW, KW)], xall.at[k, chip, rows], in_sem.at[2 + k])
            for k in range(n_k)]
    i_in = pltpu.make_async_copy(idx_ref, idxv, in_sem.at[0])
    g_in = pltpu.make_async_copy(g_ref, gv, in_sem.at[1])
    i_in.start()
    g_in.start()
    for c in x_in:
        c.start()
    barrier = pltpu.get_barrier_semaphore()
    peers = [(1, False), (2, False), (3, False), (0, True)]
    for r, flip in peers:
        pl.semaphore_signal(barrier, inc=1, device_id=dev(r, flip), device_id_type=pl.DeviceIdType.MESH)
    lax.fori_loop(0, PRIME[0], prime, 0)
    i_in.wait()
    g_in.wait()

    ids, gates = idxv[...], gv[...]
    line = lax.broadcasted_iota(jnp.int32, (2 * n_exp, t_loc), 0)
    gd = jnp.zeros((2 * n_exp, t_loc), F32)
    hit = jnp.zeros((2 * n_exp, t_loc), F32)
    for j in range(top):
        eq = ids[j:j + 1] == line
        gd = jnp.where(eq, gates[j:j + 1], gd)
        hit = jnp.where(eq, 1.0, hit)
    before = (lax.broadcasted_iota(jnp.int32, (t_loc, t_loc), 0)
              < lax.broadcasted_iota(jnp.int32, (t_loc, t_loc), 1)).astype(BF16)
    slot = _dot(hit.astype(BF16), before)
    keep = jnp.logical_and(hit > 0.5, slot < cap - 0.5)
    sall[chip, rows] = jnp.where(keep, slot, -1.0).T.astype(BF16)
    gall[chip, rows] = jnp.where(keep, gd, 0.0).T

    for c in x_in:
        c.wait()
    pl.semaphore_wait(barrier, len(peers))

    def block(buf, r, k, mine=True):
        at = buf if k is None else buf.at[k]
        return at.at[chip_of(r), rows if mine else other]

    def send(buf, ss, rs, ps, k, to=(3, 1, 2, 0)):
        for r in to:
            ref = block(buf, 0, k)
            remote(ref, ref, ss, rs.at[r] if r else ps.at[0], dev(r, r == 0)).start()

    def forward(buf, ss, rs, ps, k):
        for r in (2, 3, 1):
            ref = block(buf, r, k)
            remote(ref, ref, ss, rs.at[r], dev(r, False)).wait_recv()
            remote(ref, ref, ss, ps.at[r], dev(0, True)).start()

    def settle(buf, ss, ps, k, froms):
        for r in froms:
            ref = block(buf, r, k, False)
            remote(ref, ref, ss, ps.at[r], dev(0, True)).wait_recv()

    sg = (sall, s_sem.at[0], sr_sem, sp_sem, None)
    gg = (gall, g_sem.at[0], gr_sem, gp_sem, None)
    xs = [(xall, x_sem.at[0], xr_sem.at[k], xp_sem.at[k], k) for k in range(n_k)]
    send(*sg)
    for x in xs:
        send(*x)
    send(*gg)
    lax.fori_loop(PRIME[0], PRIME[1], prime, 0)

    pair = 2 * t_loc
    nk = n_el * 2 * cap
    m = 8 * cap
    el = lax.broadcasted_iota(jnp.int32, (2 * n_exp, nk), 1) // (2 * cap) + ep * n_el
    expand = (lax.broadcasted_iota(jnp.int32, (2 * n_exp, nk), 0) == el).astype(BF16)
    kl = lax.broadcasted_iota(jnp.int32, (pair, nk), 1)
    tr = lax.broadcasted_iota(jnp.int32, (pair, nk), 0)
    want = jnp.where(lax.rem(kl // cap, 2) == tr // t_loc, lax.rem(kl, cap), -2).astype(F32)

    def plan(r):
        q = chip_of(r)
        pt[q] = jnp.where(_dot(sall[q], expand) == want, 1.0, 0.0).T.astype(BF16)

    def dispatch(k, r):
        q = chip_of(r)
        got = _dot(pt[q], xall[k, q])
        xg[k, :, q] = got.astype(BF16).reshape(n_el, 2 * cap, KW)

    settle(sall, s_sem.at[0], sp_sem, None, (0,))
    for x in xs:
        settle(xall, x_sem.at[0], x[3], x[4], (0,))
    plan(0)
    for k in range(n_k):
        dispatch(k, 0)
    lax.fori_loop(PRIME[1], PRIME[2], prime, 0)
    forward(*sg)
    settle(sall, s_sem.at[0], sp_sem, None, (2, 3, 1))
    for r in (2, 3, 1):
        plan(r)
    lax.fori_loop(PRIME[2], PRIME[3], prime, 0)

    always = dp >= 0

    def own(v, e):
        return jnp.where(always, v[:m], v[m:]) if e % 2 == 0 else jnp.where(always, v[m:], v[:m])

    def swiglu(v):
        a, b = v[:, :fl], v[:, fl:]
        return (a * jax.nn.sigmoid(a) * b).astype(BF16)

    forward(*xs[0])
    for p in range(NW // 2):
        wait(p)
    acc[...] = jnp.zeros_like(acc)
    nt = KW // kd

    def stage(k, _):
        settle(xall, x_sem.at[0], xp_sem.at[k], k, (2, 3, 1))

        @pl.when(k + 1 < n_k)
        def _():
            forward(xall, x_sem.at[0], xr_sem.at[k + 1], xp_sem.at[k + 1], k + 1)

        start(PRIME[3] + k)
        for r in (2, 3, 1):
            dispatch(k, r)
        for e in range(NW):
            w = ring[e // 2, e % 2, pl.ds(k * nt, nt)].reshape(KW, 2 * fl)
            acc[e] += own(_dot(xg[k, e // 2 * 2:e // 2 * 2 + 2].reshape(2 * m, KW), w), e)
        return 0

    lax.fori_loop(0, n_k, stage, 0)
    forward(*gg)
    for e in range(NW):
        hbuf[e] = swiglu(acc[e])
    for p in range(3):
        start(p + NP)

    settle(gall, g_sem.at[0], gp_sem, None, (0, 2, 3, 1))
    here = (_dot(sall[...].reshape(4 * pair, 2 * n_exp), expand).reshape(4, pair, nk) == want)
    gs = gall[...].reshape(4 * pair, 2 * n_exp)
    hi = gs.astype(BF16)
    r1 = gs - hi.astype(F32)
    mid = r1.astype(BF16)
    lo = (r1 - mid.astype(F32)).astype(BF16)
    for k, p in enumerate((hi, mid, lo)):
        gt[:, pl.ds(k * pair, pair)] = jnp.where(here, _dot(p, expand).reshape(4, pair, nk), 0.0).astype(BF16)

    def up(u, _):
        start(NP + 3 + u - NW // UP)
        for j in range(UP // 2):
            wait(u * (UP // 2) + j)
        for j in range(UP):
            w = ring[lax.rem(u * (UP // 2) + j // 2, NP), j % 2].reshape(n_k, KW, 2 * fl)
            two = pl.ds(u * UP + j // 2 * 2, 2)
            v = _dot(xg[0, two].reshape(2 * m, KW), w[0])
            for k in range(1, n_k):
                v = v + _dot(xg[k, two].reshape(2 * m, KW), w[k])
            hbuf[u * UP + j] = swiglu(own(v, j))
        return 0

    lax.fori_loop(NW // UP, n_el // UP, up, 0)

    wait_bytes(xall.at[pl.ds(0, n_k - 1)], x_sem.at[0])
    wait_bytes(xall.at[0, pl.ds(0, n_k // 2)], x_sem.at[0])
    for buf, sem in ((sall, s_sem), (gall, g_sem)):
        wait_bytes(buf.at[pl.ds(0, 3)], sem.at[0])
        wait_bytes(buf.at[0, pl.ds(0, t_loc)], sem.at[0])

    def y_copy(c):
        return remote(yacc.at[c, 1 - core], yrecv.at[c], y_sem.at[0], yr_sem.at[c], dev(0, True))

    def second(c):
        y_copy(c).wait_recv()
        ssum[c] = yacc[c, core] + yrecv[c]
        for r in (3, 1, 2):
            remote(ssum.at[c, chip_of(r)], rfin.at[c, r - 1], z_sem.at[0], zr_sem.at[c], dev(r, False)).start()

    def products(c):
        for e in range(n_el):
            i, j = e // 8, e % 8
            w = ring[lax.rem(c + n_w13, NP), i % 2, j, :, (i // 2) * CW:(i // 2 + 1) * CW]
            y = own(_dot(hbuf[e // 2 * 2:e // 2 * 2 + 2].reshape(2 * m, fl), w), e)
            ybuf[lax.rem(c, 2), e] = y.astype(BF16).reshape(4, 2 * cap, CW)

    def combine(c):
        for p in range(4):
            z = _dot(gt[p], ybuf[lax.rem(c, 2), :, p].reshape(nk, CW))
            z = z[:pair] + z[pair:2 * pair] + z[2 * pair:]
            for k in range(2):
                yacc[c, k, p] = z[k * t_loc:(k + 1) * t_loc]

    def down(c, _):
        start(NP + 3 + n_el // UP - NW // UP + c)
        wait(n_w13 + c)
        combine(lax.rem(c + n_chunk - 1, n_chunk))
        products(c)

        @pl.when(c > 0)
        def _():
            y_copy(c - 1).start()

        @pl.when(c > 1)
        def _():
            second(c - 2)

        return 0

    lax.fori_loop(0, n_chunk, down, 0)
    combine(n_chunk - 1)
    second(n_chunk - 2)
    y_copy(n_chunk - 1).start()

    def total(c):
        wait_bytes(rfin.at[c], zr_sem.at[c])
        o_ref[:, pl.ds(pl.multiple_of(c * CW, CW), CW)] = ssum[c, chip] + rfin[c, 0] + rfin[c, 1] + rfin[c, 2]

    for c in range(n_chunk - 4):
        total(c)
    second(n_chunk - 1)
    for c in range(n_chunk - 4, n_chunk):
        total(c)
    wait_bytes(yrecv, y_sem.at[0])
    wait_bytes(rfin, z_sem.at[0])


def solution(mesh):
    rows = P(("dp", "ep", "tp"), None)

    def local(x, idx, g, w1, w3, w2):
        t_loc, d = x.shape
        top = idx.shape[1]
        el, _, fl = w1.shape
        n_exp = 2 * el
        cap = CF * top * t_loc // n_exp
        nc = d // CW
        nk = el * 2 * cap
        dma, vm = pltpu.SemaphoreType.DMA, pltpu.VMEM
        any_ = pl.BlockSpec(memory_space=pl.ANY)
        y = pl.pallas_call(
            functools.partial(_kernel, el, cap),
            out_shape=jax.ShapeDtypeStruct((t_loc, d), F32),
            in_specs=[any_] * 6,
            out_specs=pl.BlockSpec(memory_space=pltpu.VMEM),
            scratch_shapes=[
                vm((d // KW, 4, 2 * t_loc, KW), BF16),
                vm((top, t_loc), jnp.int32),
                vm((top, t_loc), F32),
                vm((4, 2 * t_loc, 2 * n_exp), BF16),
                vm((4, 2 * t_loc, 2 * n_exp), F32),
                vm((d // KW, el, 4, 2 * cap, KW), BF16),
                vm((NP, 2, d // fl, fl, 2 * fl), BF16),
                vm((NW, 8 * cap, 2 * fl), F32),
                vm((el, 8 * cap, fl), BF16),
                vm((4, 6 * t_loc, nk), BF16),
                vm((4, nk, 2 * t_loc), BF16),
                vm((2, el, 4, 2 * cap, CW), BF16),
                vm((nc, 2, 4, t_loc, CW), F32),
                vm((nc, 4, t_loc, CW), F32),
                vm((nc, 4, t_loc, CW), F32),
                vm((nc, 3, t_loc, CW), F32),
                dma((2 + d // KW,)), dma((NP,)),
                dma((1,)), dma((d // KW, 4)), dma((d // KW, 4)),
                dma((1,)), dma((4,)), dma((4,)),
                dma((1,)), dma((4,)), dma((4,)),
                dma((1,)), dma((nc,)), dma((1,)), dma((nc,)),
            ],
            compiler_params=pltpu.CompilerParams(collective_id=0, has_side_effects=True,
                                                 vmem_limit_bytes=67043328),
            name="moe",
        )(x, idx.T, g.T, w1.reshape(el, d // fl, fl, fl), w3.reshape(el, d // fl, fl, fl),
          w2.reshape(el // 8, 8, fl, d))
        return y.astype(BF16)

    return jax.shard_map(local, mesh=mesh,
                         in_specs=(rows, rows, rows, P("ep", None, "tp"), P("ep", None, "tp"), P("ep", "tp", None)),
                         out_specs=rows, check_vma=False)
```

```python
import functools

import jax
import jax.numpy as jnp
from jax import lax
from jax.experimental import pallas as pl
from jax.experimental.pallas import tpu as pltpu
from jax.sharding import PartitionSpec as P

CF = 2
NP = 10
PRIME = (4, 6, 8, NP)
KW = 512
NW = 8
UP = 4
CW = 256
F32, BF16 = jnp.float32, jnp.bfloat16


def _dot(a, b):
    return jnp.dot(a, b, preferred_element_type=F32)


def _kernel(n_el, cap, x_ref, idx_ref, g_ref, w1_ref, w3_ref, w2_ref, o_ref,
            xall, idxv, gv, sall, gall, xg, ring, acc, hbuf, gt, pt, ybuf, yacc, yrecv, ssum, rfin,
            in_sem, wsem, x_sem, xr_sem, xp_sem, s_sem, sr_sem, sp_sem, g_sem, gr_sem, gp_sem, y_sem, yr_sem, z_sem, zr_sem, obuf, o_sem):
    ep, tp = lax.axis_index("ep"), lax.axis_index("tp")
    dp = lax.axis_index("dp")
    core = lax.rem(tp, 2)
    chip = ep * 2 + tp // 2
    t_loc, d = x_ref.shape
    top = idx_ref.shape[0]
    n_exp = 2 * n_el
    n_chunk = d // CW
    kd, fl = w1_ref.shape[2], w1_ref.shape[3]
    n_k = d // KW
    n_w13 = n_el // 2
    n_pair = n_w13 + n_chunk
    rows = pl.ds(core * t_loc, t_loc)
    other = pl.ds((1 - core) * t_loc, t_loc)

    def dev(r, flip):
        e2 = 1 - ep if r & 2 else ep
        x2 = 1 - tp // 2 if r & 1 else tp // 2
        c2 = 1 - core if flip else core
        return (dp, e2, x2 * 2 + c2)

    def chip_of(r):
        e2 = 1 - ep if r & 2 else ep
        x2 = 1 - tp // 2 if r & 1 else tp // 2
        return e2 * 2 + x2

    def remote(src, dst, ss, rs, to):
        return pltpu.make_async_remote_copy(src_ref=src, dst_ref=dst, send_sem=ss, recv_sem=rs, device_id=to,
                                            device_id_type=pl.DeviceIdType.MESH)

    def wait_bytes(ref, sem):
        pltpu.make_async_copy(ref, ref, sem).wait()

    def start(p):
        slot = lax.rem(p, NP)
        left, right = pl.ds(0, fl), pl.ds(fl, fl)

        @pl.when(p < n_w13)
        def _():
            for i in range(2):
                for w, half in ((w1_ref, left), (w3_ref, right)):
                    for h in range(2):
                        part = pl.ds(h * 4, 4)
                        pltpu.make_async_copy(w.at[2 * p + i, part], ring.at[slot, i, part, :, half],
                                              wsem.at[slot]).start()

        @pl.when(jnp.logical_and(p >= n_w13, p < n_pair))
        def _():
            cols = pl.ds(pl.multiple_of((p - n_w13) * CW, CW), CW)
            for i in range(2):
                for k, half in enumerate((left, right)):
                    for h in range(2):
                        part = pl.ds(h * 4, 4)
                        pltpu.make_async_copy(w2_ref.at[2 * k + i, part, :, cols], ring.at[slot, i, part, :, half],
                                              wsem.at[slot]).start()

    def wait(p):
        slot = lax.rem(p, NP)
        wait_bytes(ring.at[slot], wsem.at[slot])

    def prime(p, _):
        start(p)
        return 0

    x_in = [pltpu.make_async_copy(x_ref.at[:, pl.ds(k * KW, KW)], xall.at[k, chip, rows], in_sem.at[2 + k])
            for k in range(n_k)]
    i_in = pltpu.make_async_copy(idx_ref, idxv, in_sem.at[0])
    g_in = pltpu.make_async_copy(g_ref, gv, in_sem.at[1])
    i_in.start()
    g_in.start()
    for c in x_in:
        c.start()
    barrier = pltpu.get_barrier_semaphore()
    peers = [(1, False), (2, False), (3, False), (0, True)]
    for r, flip in peers:
        pl.semaphore_signal(barrier, inc=1, device_id=dev(r, flip), device_id_type=pl.DeviceIdType.MESH)
    lax.fori_loop(0, PRIME[0], prime, 0)
    i_in.wait()
    g_in.wait()

    ids, gates = idxv[...], gv[...]
    line = lax.broadcasted_iota(jnp.int32, (2 * n_exp, t_loc), 0)
    gd = jnp.zeros((2 * n_exp, t_loc), F32)
    hit = jnp.zeros((2 * n_exp, t_loc), F32)
    for j in range(top):
        eq = ids[j:j + 1] == line
        gd = jnp.where(eq, gates[j:j + 1], gd)
        hit = jnp.where(eq, 1.0, hit)
    before = (lax.broadcasted_iota(jnp.int32, (t_loc, t_loc), 0)
              < lax.broadcasted_iota(jnp.int32, (t_loc, t_loc), 1)).astype(BF16)
    slot = _dot(hit.astype(BF16), before)
    keep = jnp.logical_and(hit > 0.5, slot < cap - 0.5)
    sall[chip, rows] = jnp.where(keep, slot, -1.0).T.astype(BF16)
    gall[chip, rows] = jnp.where(keep, gd, 0.0).T

    for c in x_in:
        c.wait()
    pl.semaphore_wait(barrier, len(peers))

    def block(buf, r, k, mine=True):
        at = buf if k is None else buf.at[k]
        return at.at[chip_of(r), rows if mine else other]

    def send(buf, ss, rs, ps, k, to=(3, 1, 2, 0)):
        for r in to:
            ref = block(buf, 0, k)
            remote(ref, ref, ss, rs.at[r] if r else ps.at[0], dev(r, r == 0)).start()

    def forward(buf, ss, rs, ps, k):
        for r in (2, 3, 1):
            ref = block(buf, r, k)
            remote(ref, ref, ss, rs.at[r], dev(r, False)).wait_recv()
            remote(ref, ref, ss, ps.at[r], dev(0, True)).start()

    def settle(buf, ss, ps, k, froms):
        for r in froms:
            ref = block(buf, r, k, False)
            remote(ref, ref, ss, ps.at[r], dev(0, True)).wait_recv()

    sg = (sall, s_sem.at[0], sr_sem, sp_sem, None)
    gg = (gall, g_sem.at[0], gr_sem, gp_sem, None)
    xs = [(xall, x_sem.at[0], xr_sem.at[k], xp_sem.at[k], k) for k in range(n_k)]
    send(*sg)
    for x in xs:
        send(*x)
    send(*gg)
    lax.fori_loop(PRIME[0], PRIME[1], prime, 0)

    pair = 2 * t_loc
    nk = n_el * 2 * cap
    m = 8 * cap
    el = lax.broadcasted_iota(jnp.int32, (2 * n_exp, nk), 1) // (2 * cap) + ep * n_el
    expand = (lax.broadcasted_iota(jnp.int32, (2 * n_exp, nk), 0) == el).astype(BF16)
    kl = lax.broadcasted_iota(jnp.int32, (pair, nk), 1)
    tr = lax.broadcasted_iota(jnp.int32, (pair, nk), 0)
    want = jnp.where(lax.rem(kl // cap, 2) == tr // t_loc, lax.rem(kl, cap), -2).astype(F32)

    def plan(r):
        q = chip_of(r)
        pt[q] = jnp.where(_dot(sall[q], expand) == want, 1.0, 0.0).T.astype(BF16)

    def dispatch(k, r):
        q = chip_of(r)
        got = _dot(pt[q], xall[k, q])
        xg[k, :, q] = got.astype(BF16).reshape(n_el, 2 * cap, KW)

    settle(sall, s_sem.at[0], sp_sem, None, (0,))
    for x in xs:
        settle(xall, x_sem.at[0], x[3], x[4], (0,))
    plan(0)
    for k in range(n_k):
        dispatch(k, 0)
    lax.fori_loop(PRIME[1], PRIME[2], prime, 0)
    forward(*sg)
    forward(*xs[0])
    settle(sall, s_sem.at[0], sp_sem, None, (2, 3, 1))
    for r in (2, 3, 1):
        plan(r)
    lax.fori_loop(PRIME[2], PRIME[3], prime, 0)

    always = dp >= 0

    def own(v, e):
        return jnp.where(always, v[:m], v[m:]) if e % 2 == 0 else jnp.where(always, v[m:], v[:m])

    def swiglu(v):
        a, b = v[:, :fl], v[:, fl:]
        return (a * jax.nn.sigmoid(a) * b).astype(BF16)

    for p in range(NW // 2):
        wait(p)
    acc[...] = jnp.zeros_like(acc)
    nt = KW // kd

    def stage(k, _):
        settle(xall, x_sem.at[0], xp_sem.at[k], k, (2, 3, 1))

        @pl.when(k + 1 < n_k)
        def _():
            forward(xall, x_sem.at[0], xr_sem.at[k + 1], xp_sem.at[k + 1], k + 1)

        for r in (2, 3, 1):
            dispatch(k, r)
        for e in range(NW):
            w = ring[e // 2, e % 2, pl.ds(k * nt, nt)].reshape(KW, 2 * fl)
            acc[e] += own(_dot(xg[k, e // 2 * 2:e // 2 * 2 + 2].reshape(2 * m, KW), w), e)
        return 0

    lax.fori_loop(0, n_k, stage, 0)
    forward(*gg)
    for e in range(NW):
        hbuf[e] = swiglu(acc[e])
    for p in range(NW // 2):
        start(p + NP)

    settle(gall, g_sem.at[0], gp_sem, None, (0, 2, 3, 1))
    here = (_dot(sall[...].reshape(4 * pair, 2 * n_exp), expand).reshape(4, pair, nk) == want)
    gs = gall[...].reshape(4 * pair, 2 * n_exp)
    hi = gs.astype(BF16)
    r1 = gs - hi.astype(F32)
    mid = r1.astype(BF16)
    lo = (r1 - mid.astype(F32)).astype(BF16)
    for k, p in enumerate((hi, mid, lo)):
        gt[:, pl.ds(k * pair, pair)] = jnp.where(here, _dot(p, expand).reshape(4, pair, nk), 0.0).astype(BF16)

    def up(u, _):
        for j in range(UP // 2):
            wait(u * (UP // 2) + j)
        for j in range(UP):
            w = ring[lax.rem(u * (UP // 2) + j // 2, NP), j % 2].reshape(n_k, KW, 2 * fl)
            two = pl.ds(u * UP + j // 2 * 2, 2)
            v = _dot(xg[0, two].reshape(2 * m, KW), w[0])
            for k in range(1, n_k):
                v = v + _dot(xg[k, two].reshape(2 * m, KW), w[k])
            hbuf[u * UP + j] = swiglu(own(v, j))
        for j in range(UP // 2):
            start(u * (UP // 2) + j + NP)
        return 0

    lax.fori_loop(NW // UP, n_el // UP, up, 0)

    wait_bytes(xall.at[pl.ds(0, n_k - 1)], x_sem.at[0])
    wait_bytes(xall.at[0, pl.ds(0, n_k // 2)], x_sem.at[0])
    for buf, sem in ((sall, s_sem), (gall, g_sem)):
        wait_bytes(buf.at[pl.ds(0, 3)], sem.at[0])
        wait_bytes(buf.at[0, pl.ds(0, t_loc)], sem.at[0])

    def y_copy(c):
        return remote(yacc.at[c, 1 - core], yrecv.at[c], y_sem.at[0], yr_sem.at[c], dev(0, True))

    def second(c):
        y_copy(c).wait_recv()
        ssum[c] = yacc[c, core] + yrecv[c]
        for r in (3, 1, 2):
            remote(ssum.at[c, chip_of(r)], rfin.at[c, r - 1], z_sem.at[0], zr_sem.at[c], dev(r, False)).start()

    def products(c):
        for e in range(n_el):
            i, j = e // 8, e % 8
            w = ring[lax.rem(c + n_w13, NP), i % 2, j, :, (i // 2) * CW:(i // 2 + 1) * CW]
            y = own(_dot(hbuf[e // 2 * 2:e // 2 * 2 + 2].reshape(2 * m, fl), w), e)
            ybuf[e] = y.astype(BF16).reshape(4, 2 * cap, CW)

    def combine(c):
        for p in range(4):
            z = _dot(gt[p], ybuf[:, p].reshape(nk, CW))
            z = z[:pair] + z[pair:2 * pair] + z[2 * pair:]
            for k in range(2):
                yacc[c, k, p] = z[k * t_loc:(k + 1) * t_loc]

    def down(c, _):
        wait(n_w13 + c)
        products(c)
        combine(c)
        y_copy(c).start()

        @pl.when(c > 0)
        def _():
            second(c - 1)

        @pl.when(c > 4)
        def _():
            total(c - 5)

        return 0

    def o_copy(c):
        cols = pl.ds(pl.multiple_of(c * CW, CW), CW)
        return pltpu.make_async_copy(obuf.at[:, cols], o_ref.at[:, cols], o_sem.at[c])

    def total(c):
        wait_bytes(rfin.at[c], zr_sem.at[c])
        cols = pl.ds(pl.multiple_of(c * CW, CW), CW)
        obuf[:, cols] = ssum[c, chip] + rfin[c, 0] + rfin[c, 1] + rfin[c, 2]
        o_copy(c).start()

    lax.fori_loop(0, n_chunk, down, 0)
    second(n_chunk - 1)
    for c in range(n_chunk - 5, n_chunk):
        total(c)
    for c in range(n_chunk):
        o_copy(c).wait()
    wait_bytes(yrecv, y_sem.at[0])
    wait_bytes(rfin, z_sem.at[0])


def solution(mesh):
    rows = P(("dp", "ep", "tp"), None)

    def local(x, idx, g, w1, w3, w2):
        t_loc, d = x.shape
        top = idx.shape[1]
        el, _, fl = w1.shape
        n_exp = 2 * el
        cap = CF * top * t_loc // n_exp
        nc = d // CW
        nk = el * 2 * cap
        dma, vm = pltpu.SemaphoreType.DMA, pltpu.VMEM
        any_ = pl.BlockSpec(memory_space=pl.ANY)
        y = pl.pallas_call(
            functools.partial(_kernel, el, cap),
            out_shape=jax.ShapeDtypeStruct((t_loc, d), F32),
            in_specs=[any_] * 6,
            out_specs=any_,
            scratch_shapes=[
                vm((d // KW, 4, 2 * t_loc, KW), BF16),
                vm((top, t_loc), jnp.int32),
                vm((top, t_loc), F32),
                vm((4, 2 * t_loc, 2 * n_exp), BF16),
                vm((4, 2 * t_loc, 2 * n_exp), F32),
                vm((d // KW, el, 4, 2 * cap, KW), BF16),
                vm((NP, 2, d // fl, fl, 2 * fl), BF16),
                vm((NW, 8 * cap, 2 * fl), F32),
                vm((el, 8 * cap, fl), BF16),
                vm((4, 6 * t_loc, nk), BF16),
                vm((4, nk, 2 * t_loc), BF16),
                vm((el, 4, 2 * cap, CW), BF16),
                vm((nc, 2, 4, t_loc, CW), F32),
                vm((nc, 4, t_loc, CW), F32),
                vm((nc, 4, t_loc, CW), F32),
                vm((nc, 3, t_loc, CW), F32),
                dma((2 + d // KW,)), dma((NP,)),
                dma((1,)), dma((d // KW, 4)), dma((d // KW, 4)),
                dma((1,)), dma((4,)), dma((4,)),
                dma((1,)), dma((4,)), dma((4,)),
                dma((1,)), dma((nc,)), dma((1,)), dma((nc,)),
                vm((t_loc, d), F32), dma((nc,)),
            ],
            compiler_params=pltpu.CompilerParams(collective_id=0, has_side_effects=True,
                                                 vmem_limit_bytes=67043328),
            name="moe",
        )(x, idx.T, g.T, w1.reshape(el, d // fl, fl, fl), w3.reshape(el, d // fl, fl, fl),
          w2.reshape(el // 8, 8, fl, d))
        return y.astype(BF16)

    return jax.shard_map(local, mesh=mesh,
                         in_specs=(rows, rows, rows, P("ep", None, "tp"), P("ep", None, "tp"), P("ep", "tp", None)),
                         out_specs=rows, check_vma=False)
```

```python
import functools

import jax
import jax.numpy as jnp
from jax import lax
from jax.experimental import pallas as pl
from jax.experimental.pallas import tpu as pltpu
from jax.sharding import PartitionSpec as P

CF = 2
NP = 11
PRIME = (4, 6, 8, NP)
KW = 512
NW = 8
UP = 4
CW = 256
F32, BF16 = jnp.float32, jnp.bfloat16


def _dot(a, b):
    return jnp.dot(a, b, preferred_element_type=F32)


def _kernel(n_el, cap, x_ref, idx_ref, g_ref, w1_ref, w3_ref, w2_ref, o_ref,
            xall, idxv, gv, sall, gall, xg, ring, acc, hbuf, gt, pt, ybuf, yacc, yrecv, rfin,
            in_sem, wsem, x_sem, xr_sem, xp_sem, s_sem, sr_sem, sp_sem, g_sem, gr_sem, gp_sem, y_sem, yr_sem, z_sem, zr_sem, obuf, o_sem):
    ep, tp = lax.axis_index("ep"), lax.axis_index("tp")
    dp = lax.axis_index("dp")
    core = lax.rem(tp, 2)
    chip = ep * 2 + tp // 2
    t_loc, d = x_ref.shape
    top = idx_ref.shape[0]
    n_exp = 2 * n_el
    n_chunk = d // CW
    kd, fl = w1_ref.shape[2], w1_ref.shape[3]
    n_k = d // KW
    n_w13 = n_el // 2
    n_pair = n_w13 + n_chunk
    rows = pl.ds(core * t_loc, t_loc)
    other = pl.ds((1 - core) * t_loc, t_loc)

    def dev(r, flip):
        e2 = 1 - ep if r & 2 else ep
        x2 = 1 - tp // 2 if r & 1 else tp // 2
        c2 = 1 - core if flip else core
        return (dp, e2, x2 * 2 + c2)

    def chip_of(r):
        e2 = 1 - ep if r & 2 else ep
        x2 = 1 - tp // 2 if r & 1 else tp // 2
        return e2 * 2 + x2

    def remote(src, dst, ss, rs, to):
        return pltpu.make_async_remote_copy(src_ref=src, dst_ref=dst, send_sem=ss, recv_sem=rs, device_id=to,
                                            device_id_type=pl.DeviceIdType.MESH)

    def wait_bytes(ref, sem):
        pltpu.make_async_copy(ref, ref, sem).wait()

    def start(p):
        slot = lax.rem(p, NP)
        left, right = pl.ds(0, fl), pl.ds(fl, fl)

        @pl.when(p < n_w13)
        def _():
            for i in range(2):
                for w, half in ((w1_ref, left), (w3_ref, right)):
                    for h in range(2):
                        part = pl.ds(h * 4, 4)
                        pltpu.make_async_copy(w.at[2 * p + i, part], ring.at[slot, i, part, :, half],
                                              wsem.at[slot]).start()

        @pl.when(jnp.logical_and(p >= n_w13, p < n_pair))
        def _():
            cols = pl.ds(pl.multiple_of((p - n_w13) * CW, CW), CW)
            for i in range(2):
                for k, half in enumerate((left, right)):
                    for h in range(2):
                        part = pl.ds(h * 4, 4)
                        pltpu.make_async_copy(w2_ref.at[2 * k + i, part, :, cols], ring.at[slot, i, part, :, half],
                                              wsem.at[slot]).start()

    def wait(p):
        slot = lax.rem(p, NP)
        wait_bytes(ring.at[slot], wsem.at[slot])

    def prime(p, _):
        start(p)
        return 0

    x_in = [pltpu.make_async_copy(x_ref.at[:, pl.ds(k * KW, KW)], xall.at[k, chip, rows], in_sem.at[2 + k])
            for k in range(n_k)]
    i_in = pltpu.make_async_copy(idx_ref, idxv, in_sem.at[0])
    g_in = pltpu.make_async_copy(g_ref, gv, in_sem.at[1])
    i_in.start()
    g_in.start()
    for c in x_in:
        c.start()
    barrier = pltpu.get_barrier_semaphore()
    peers = [(1, False), (2, False), (3, False), (0, True)]
    for r, flip in peers:
        pl.semaphore_signal(barrier, inc=1, device_id=dev(r, flip), device_id_type=pl.DeviceIdType.MESH)
    lax.fori_loop(0, PRIME[0], prime, 0)
    i_in.wait()
    g_in.wait()

    ids, gates = idxv[...], gv[...]
    line = lax.broadcasted_iota(jnp.int32, (2 * n_exp, t_loc), 0)
    gd = jnp.zeros((2 * n_exp, t_loc), F32)
    hit = jnp.zeros((2 * n_exp, t_loc), F32)
    for j in range(top):
        eq = ids[j:j + 1] == line
        gd = jnp.where(eq, gates[j:j + 1], gd)
        hit = jnp.where(eq, 1.0, hit)
    before = (lax.broadcasted_iota(jnp.int32, (t_loc, t_loc), 0)
              < lax.broadcasted_iota(jnp.int32, (t_loc, t_loc), 1)).astype(BF16)
    slot = _dot(hit.astype(BF16), before)
    keep = jnp.logical_and(hit > 0.5, slot < cap - 0.5)
    sall[chip, rows] = jnp.where(keep, slot, -1.0).T.astype(BF16)
    gall[chip, rows] = jnp.where(keep, gd, 0.0).T

    for c in x_in:
        c.wait()
    pl.semaphore_wait(barrier, len(peers))

    def block(buf, r, k, mine=True):
        at = buf if k is None else buf.at[k]
        return at.at[chip_of(r), rows if mine else other]

    def send(buf, ss, rs, ps, k, to=(3, 1, 2, 0)):
        for r in to:
            ref = block(buf, 0, k)
            remote(ref, ref, ss, rs.at[r] if r else ps.at[0], dev(r, r == 0)).start()

    def forward(buf, ss, rs, ps, k):
        for r in (2, 3, 1):
            ref = block(buf, r, k)
            remote(ref, ref, ss, rs.at[r], dev(r, False)).wait_recv()
            remote(ref, ref, ss, ps.at[r], dev(0, True)).start()

    def settle(buf, ss, ps, k, froms):
        for r in froms:
            ref = block(buf, r, k, False)
            remote(ref, ref, ss, ps.at[r], dev(0, True)).wait_recv()

    sg = (sall, s_sem.at[0], sr_sem, sp_sem, None)
    gg = (gall, g_sem.at[0], gr_sem, gp_sem, None)
    xs = [(xall, x_sem.at[0], xr_sem.at[k], xp_sem.at[k], k) for k in range(n_k)]
    send(*sg)
    for x in xs:
        send(*x)
    send(*gg)
    lax.fori_loop(PRIME[0], PRIME[1], prime, 0)

    pair = 2 * t_loc
    nk = n_el * 2 * cap
    m = 8 * cap
    el = lax.broadcasted_iota(jnp.int32, (2 * n_exp, nk), 1) // (2 * cap) + ep * n_el
    expand = (lax.broadcasted_iota(jnp.int32, (2 * n_exp, nk), 0) == el).astype(BF16)
    kl = lax.broadcasted_iota(jnp.int32, (pair, nk), 1)
    tr = lax.broadcasted_iota(jnp.int32, (pair, nk), 0)
    want = jnp.where(lax.rem(kl // cap, 2) == tr // t_loc, lax.rem(kl, cap), -2).astype(F32)

    def plan(r):
        q = chip_of(r)
        pt[q] = jnp.where(_dot(sall[q], expand) == want, 1.0, 0.0).T.astype(BF16)

    def dispatch(k, r):
        q = chip_of(r)
        got = _dot(pt[q], xall[k, q])
        xg[k, :, q] = got.astype(BF16).reshape(n_el, 2 * cap, KW)

    settle(sall, s_sem.at[0], sp_sem, None, (0,))
    for x in xs:
        settle(xall, x_sem.at[0], x[3], x[4], (0,))
    plan(0)
    for k in range(n_k):
        dispatch(k, 0)
    lax.fori_loop(PRIME[1], PRIME[2], prime, 0)
    forward(*sg)
    forward(*xs[0])
    settle(sall, s_sem.at[0], sp_sem, None, (2, 3, 1))
    for r in (2, 3, 1):
        plan(r)
    lax.fori_loop(PRIME[2], PRIME[3], prime, 0)

    always = dp >= 0

    def own(v, e):
        return jnp.where(always, v[:m], v[m:]) if e % 2 == 0 else jnp.where(always, v[m:], v[:m])

    def swiglu(v):
        a, b = v[:, :fl], v[:, fl:]
        return (a * jax.nn.sigmoid(a) * b).astype(BF16)

    for p in range(NW // 2):
        wait(p)
    acc[...] = jnp.zeros_like(acc)
    nt = KW // kd

    def stage(k, _):
        settle(xall, x_sem.at[0], xp_sem.at[k], k, (2, 3, 1))

        @pl.when(k + 1 < n_k)
        def _():
            forward(xall, x_sem.at[0], xr_sem.at[k + 1], xp_sem.at[k + 1], k + 1)

        for r in (2, 3, 1):
            dispatch(k, r)
        for e in range(NW):
            w = ring[e // 2, e % 2, pl.ds(k * nt, nt)].reshape(KW, 2 * fl)
            acc[e] += own(_dot(xg[k, e // 2 * 2:e // 2 * 2 + 2].reshape(2 * m, KW), w), e)
        return 0

    lax.fori_loop(0, n_k, stage, 0)
    forward(*gg)
    for e in range(NW):
        hbuf[e] = swiglu(acc[e])
    for p in range(NW // 2):
        start(p + NP)

    settle(gall, g_sem.at[0], gp_sem, None, (0, 2, 3, 1))
    here = (_dot(sall[...].reshape(4 * pair, 2 * n_exp), expand).reshape(4, pair, nk) == want)
    gs = gall[...].reshape(4 * pair, 2 * n_exp)
    hi = gs.astype(BF16)
    r1 = gs - hi.astype(F32)
    mid = r1.astype(BF16)
    lo = (r1 - mid.astype(F32)).astype(BF16)
    for k, p in enumerate((hi, mid, lo)):
        gt[:, pl.ds(k * pair, pair)] = jnp.where(here, _dot(p, expand).reshape(4, pair, nk), 0.0).astype(BF16)

    def up(u, _):
        for j in range(UP // 2):
            wait(u * (UP // 2) + j)
        for j in range(UP):
            w = ring[lax.rem(u * (UP // 2) + j // 2, NP), j % 2].reshape(n_k, KW, 2 * fl)
            two = pl.ds(u * UP + j // 2 * 2, 2)
            v = _dot(xg[0, two].reshape(2 * m, KW), w[0])
            for k in range(1, n_k):
                v = v + _dot(xg[k, two].reshape(2 * m, KW), w[k])
            hbuf[u * UP + j] = swiglu(own(v, j))
        for j in range(UP // 2):
            start(u * (UP // 2) + j + NP)
        return 0

    lax.fori_loop(NW // UP, n_el // UP, up, 0)

    wait_bytes(xall.at[pl.ds(0, n_k - 1)], x_sem.at[0])
    wait_bytes(xall.at[0, pl.ds(0, n_k // 2)], x_sem.at[0])
    for buf, sem in ((sall, s_sem), (gall, g_sem)):
        wait_bytes(buf.at[pl.ds(0, 3)], sem.at[0])
        wait_bytes(buf.at[0, pl.ds(0, t_loc)], sem.at[0])

    def y_copy(c):
        return remote(yacc.at[c, 1 - core], yrecv.at[c], y_sem.at[0], yr_sem.at[c], dev(0, True))

    def second(c):
        y_copy(c).wait_recv()
        yacc[c, core] += yrecv[c]
        for r in (3, 1, 2):
            remote(yacc.at[c, core, chip_of(r)], rfin.at[c, r - 1], z_sem.at[0], zr_sem.at[c], dev(r, False)).start()

    def products(c):
        for e in range(n_el):
            i, j = e // 8, e % 8
            w = ring[lax.rem(c + n_w13, NP), i % 2, j, :, (i // 2) * CW:(i // 2 + 1) * CW]
            y = own(_dot(hbuf[e // 2 * 2:e // 2 * 2 + 2].reshape(2 * m, fl), w), e)
            ybuf[e] = y.astype(BF16).reshape(4, 2 * cap, CW)

    def combine(c):
        for p in range(4):
            z = _dot(gt[p], ybuf[:, p].reshape(nk, CW))
            z = z[:pair] + z[pair:2 * pair] + z[2 * pair:]
            for k in range(2):
                yacc[c, k, p] = z[k * t_loc:(k + 1) * t_loc]

    def down(c, _):
        wait(n_w13 + c)
        products(c)
        combine(c)
        y_copy(c).start()

        @pl.when(c > 0)
        def _():
            second(c - 1)

        @pl.when(c > 4)
        def _():
            total(c - 5)

        return 0

    def o_copy(c):
        cols = pl.ds(pl.multiple_of(c * CW, CW), CW)
        return pltpu.make_async_copy(obuf.at[:, cols], o_ref.at[:, cols], o_sem.at[c])

    def total(c):
        wait_bytes(rfin.at[c], zr_sem.at[c])
        cols = pl.ds(pl.multiple_of(c * CW, CW), CW)
        obuf[:, cols] = (yacc[c, core, chip] + rfin[c, 0] + rfin[c, 1] + rfin[c, 2]).astype(BF16)
        o_copy(c).start()

    lax.fori_loop(0, n_chunk, down, 0)
    second(n_chunk - 1)
    for c in range(n_chunk - 5, n_chunk):
        total(c)
    for c in range(n_chunk):
        o_copy(c).wait()
    wait_bytes(yrecv, y_sem.at[0])
    wait_bytes(rfin, z_sem.at[0])


def solution(mesh):
    rows = P(("dp", "ep", "tp"), None)

    def local(x, idx, g, w1, w3, w2):
        t_loc, d = x.shape
        top = idx.shape[1]
        el, _, fl = w1.shape
        n_exp = 2 * el
        cap = CF * top * t_loc // n_exp
        nc = d // CW
        nk = el * 2 * cap
        dma, vm = pltpu.SemaphoreType.DMA, pltpu.VMEM
        any_ = pl.BlockSpec(memory_space=pl.ANY)
        y = pl.pallas_call(
            functools.partial(_kernel, el, cap),
            out_shape=jax.ShapeDtypeStruct((t_loc, d), BF16),
            in_specs=[any_] * 6,
            out_specs=any_,
            scratch_shapes=[
                vm((d // KW, 4, 2 * t_loc, KW), BF16),
                vm((top, t_loc), jnp.int32),
                vm((top, t_loc), F32),
                vm((4, 2 * t_loc, 2 * n_exp), BF16),
                vm((4, 2 * t_loc, 2 * n_exp), F32),
                vm((d // KW, el, 4, 2 * cap, KW), BF16),
                vm((NP, 2, d // fl, fl, 2 * fl), BF16),
                vm((NW, 8 * cap, 2 * fl), F32),
                vm((el, 8 * cap, fl), BF16),
                vm((4, 6 * t_loc, nk), BF16),
                vm((4, nk, 2 * t_loc), BF16),
                vm((el, 4, 2 * cap, CW), BF16),
                vm((nc, 2, 4, t_loc, CW), F32),
                vm((nc, 4, t_loc, CW), F32),
                vm((nc, 3, t_loc, CW), F32),
                dma((2 + d // KW,)), dma((NP,)),
                dma((1,)), dma((d // KW, 4)), dma((d // KW, 4)),
                dma((1,)), dma((4,)), dma((4,)),
                dma((1,)), dma((4,)), dma((4,)),
                dma((1,)), dma((nc,)), dma((1,)), dma((nc,)),
                vm((t_loc, d), BF16), dma((nc,)),
            ],
            compiler_params=pltpu.CompilerParams(collective_id=0, has_side_effects=True,
                                                 vmem_limit_bytes=67043328),
            name="moe",
        )(x, idx.T, g.T, w1.reshape(el, d // fl, fl, fl), w3.reshape(el, d // fl, fl, fl),
          w2.reshape(el // 8, 8, fl, d))
        return y

    return jax.shard_map(local, mesh=mesh,
                         in_specs=(rows, rows, rows, P("ep", None, "tp"), P("ep", None, "tp"), P("ep", "tp", None)),
                         out_specs=rows, check_vma=False)
```

```python
import functools

import jax
import jax.numpy as jnp
from jax import lax
from jax.experimental import pallas as pl
from jax.experimental.pallas import tpu as pltpu
from jax.sharding import PartitionSpec as P

CF = 2
NP = 10
PRIME = (4, 6, 8, NP)
KW = 512
NW = 8
UP = 4
CW = 256
NR = 5
F32, BF16 = jnp.float32, jnp.bfloat16


def _dot(a, b):
    return jnp.dot(a, b, preferred_element_type=F32)


def _kernel(n_el, cap, x_ref, idx_ref, g_ref, w1_ref, w3_ref, w2_ref, o_ref,
            xall, idxv, gv, sall, gall, xg, ring, acc, hbuf, gt, pt, ybuf, yacc, yrecv, rfin,
            in_sem, wsem, x_sem, xr_sem, xp_sem, s_sem, sr_sem, sp_sem, g_sem, gr_sem, gp_sem, y_sem, yr_sem, z_sem, zr_sem, obuf, o_sem, rmid, zm_sem):
    ep, tp = lax.axis_index("ep"), lax.axis_index("tp")
    dp = lax.axis_index("dp")
    core = lax.rem(tp, 2)
    chip = ep * 2 + tp // 2
    t_loc, d = x_ref.shape
    top = idx_ref.shape[0]
    n_exp = 2 * n_el
    n_chunk = d // CW
    kd, fl = w1_ref.shape[2], w1_ref.shape[3]
    n_k = d // KW
    n_w13 = n_el // 2
    n_pair = n_w13 + n_chunk
    rows = pl.ds(core * t_loc, t_loc)
    other = pl.ds((1 - core) * t_loc, t_loc)

    def dev(r, flip):
        e2 = 1 - ep if r & 2 else ep
        x2 = 1 - tp // 2 if r & 1 else tp // 2
        c2 = 1 - core if flip else core
        return (dp, e2, x2 * 2 + c2)

    def chip_of(r):
        e2 = 1 - ep if r & 2 else ep
        x2 = 1 - tp // 2 if r & 1 else tp // 2
        return e2 * 2 + x2

    def remote(src, dst, ss, rs, to):
        return pltpu.make_async_remote_copy(src_ref=src, dst_ref=dst, send_sem=ss, recv_sem=rs, device_id=to,
                                            device_id_type=pl.DeviceIdType.MESH)

    def wait_bytes(ref, sem):
        pltpu.make_async_copy(ref, ref, sem).wait()

    def start(p):
        slot = lax.rem(p, NP)
        left, right = pl.ds(0, fl), pl.ds(fl, fl)

        @pl.when(p < n_w13)
        def _():
            for i in range(2):
                for w, half in ((w1_ref, left), (w3_ref, right)):
                    for h in range(2):
                        part = pl.ds(h * 4, 4)
                        pltpu.make_async_copy(w.at[2 * p + i, part], ring.at[slot, i, part, :, half],
                                              wsem.at[slot]).start()

        @pl.when(jnp.logical_and(p >= n_w13, p < n_pair))
        def _():
            cols = pl.ds(pl.multiple_of((p - n_w13) * CW, CW), CW)
            for i in range(2):
                for k, half in enumerate((left, right)):
                    for h in range(2):
                        part = pl.ds(h * 4, 4)
                        pltpu.make_async_copy(w2_ref.at[2 * k + i, part, :, cols], ring.at[slot, i, part, :, half],
                                              wsem.at[slot]).start()

    def wait(p):
        slot = lax.rem(p, NP)
        wait_bytes(ring.at[slot], wsem.at[slot])

    def prime(p, _):
        start(p)
        return 0

    x_in = [pltpu.make_async_copy(x_ref.at[:, pl.ds(k * KW, KW)], xall.at[k, chip, rows], in_sem.at[2 + k])
            for k in range(n_k)]
    i_in = pltpu.make_async_copy(idx_ref, idxv, in_sem.at[0])
    g_in = pltpu.make_async_copy(g_ref, gv, in_sem.at[1])
    i_in.start()
    g_in.start()
    for c in x_in:
        c.start()
    barrier = pltpu.get_barrier_semaphore()
    peers = [(1, False), (2, False), (3, False), (0, True)]
    for r, flip in peers:
        pl.semaphore_signal(barrier, inc=1, device_id=dev(r, flip), device_id_type=pl.DeviceIdType.MESH)
    lax.fori_loop(0, PRIME[0], prime, 0)
    i_in.wait()
    g_in.wait()

    ids, gates = idxv[...], gv[...]
    line = lax.broadcasted_iota(jnp.int32, (2 * n_exp, t_loc), 0)
    gd = jnp.zeros((2 * n_exp, t_loc), F32)
    hit = jnp.zeros((2 * n_exp, t_loc), F32)
    for j in range(top):
        eq = ids[j:j + 1] == line
        gd = jnp.where(eq, gates[j:j + 1], gd)
        hit = jnp.where(eq, 1.0, hit)
    before = (lax.broadcasted_iota(jnp.int32, (t_loc, t_loc), 0)
              < lax.broadcasted_iota(jnp.int32, (t_loc, t_loc), 1)).astype(BF16)
    slot = _dot(hit.astype(BF16), before)
    keep = jnp.logical_and(hit > 0.5, slot < cap - 0.5)
    sall[chip, rows] = jnp.where(keep, slot, -1.0).T.astype(BF16)
    gall[chip, rows] = jnp.where(keep, gd, 0.0).T

    for c in x_in:
        c.wait()
    pl.semaphore_wait(barrier, len(peers))

    def block(buf, r, k, mine=True):
        at = buf if k is None else buf.at[k]
        return at.at[chip_of(r), rows if mine else other]

    def send(buf, ss, rs, ps, k, to=(3, 1, 2, 0)):
        for r in to:
            ref = block(buf, 0, k)
            remote(ref, ref, ss, rs.at[r] if r else ps.at[0], dev(r, r == 0)).start()

    def forward(buf, ss, rs, ps, k):
        for r in (2, 3, 1):
            ref = block(buf, r, k)
            remote(ref, ref, ss, rs.at[r], dev(r, False)).wait_recv()
            remote(ref, ref, ss, ps.at[r], dev(0, True)).start()

    def settle(buf, ss, ps, k, froms):
        for r in froms:
            ref = block(buf, r, k, False)
            remote(ref, ref, ss, ps.at[r], dev(0, True)).wait_recv()

    sg = (sall, s_sem.at[0], sr_sem, sp_sem, None)
    gg = (gall, g_sem.at[0], gr_sem, gp_sem, None)
    xs = [(xall, x_sem.at[0], xr_sem.at[k], xp_sem.at[k], k) for k in range(n_k)]
    send(*sg)
    for x in xs:
        send(*x)
    send(*gg)
    lax.fori_loop(PRIME[0], PRIME[1], prime, 0)

    pair = 2 * t_loc
    nk = n_el * 2 * cap
    m = 8 * cap
    el = lax.broadcasted_iota(jnp.int32, (2 * n_exp, nk), 1) // (2 * cap) + ep * n_el
    expand = (lax.broadcasted_iota(jnp.int32, (2 * n_exp, nk), 0) == el).astype(BF16)
    kl = lax.broadcasted_iota(jnp.int32, (pair, nk), 1)
    tr = lax.broadcasted_iota(jnp.int32, (pair, nk), 0)
    want = jnp.where(lax.rem(kl // cap, 2) == tr // t_loc, lax.rem(kl, cap), -2).astype(F32)

    def plan(r):
        q = chip_of(r)
        pt[q] = jnp.where(_dot(sall[q], expand) == want, 1.0, 0.0).T.astype(BF16)

    def dispatch(k, r):
        q = chip_of(r)
        got = _dot(pt[q], xall[k, q])
        xg[k, :, q] = got.astype(BF16).reshape(n_el, 2 * cap, KW)

    settle(sall, s_sem.at[0], sp_sem, None, (0,))
    for x in xs:
        settle(xall, x_sem.at[0], x[3], x[4], (0,))
    plan(0)
    for k in range(n_k):
        dispatch(k, 0)
    lax.fori_loop(PRIME[1], PRIME[2], prime, 0)
    forward(*sg)
    forward(*xs[0])
    settle(sall, s_sem.at[0], sp_sem, None, (2, 3, 1))
    for r in (2, 3, 1):
        plan(r)
    lax.fori_loop(PRIME[2], PRIME[3], prime, 0)

    always = dp >= 0

    def own(v, e):
        return jnp.where(always, v[:m], v[m:]) if e % 2 == 0 else jnp.where(always, v[m:], v[:m])

    def swiglu(v):
        a, b = v[:, :fl], v[:, fl:]
        return (a * jax.nn.sigmoid(a) * b).astype(BF16)

    for p in range(NW // 2):
        wait(p)
    acc[...] = jnp.zeros_like(acc)
    nt = KW // kd

    def stage(k, _):
        settle(xall, x_sem.at[0], xp_sem.at[k], k, (2, 3, 1))

        @pl.when(k + 1 < n_k)
        def _():
            forward(xall, x_sem.at[0], xr_sem.at[k + 1], xp_sem.at[k + 1], k + 1)

        for r in (2, 3, 1):
            dispatch(k, r)
        for e in range(NW):
            w = ring[e // 2, e % 2, pl.ds(k * nt, nt)].reshape(KW, 2 * fl)
            acc[e] += own(_dot(xg[k, e // 2 * 2:e // 2 * 2 + 2].reshape(2 * m, KW), w), e)
        return 0

    lax.fori_loop(0, n_k, stage, 0)
    forward(*gg)
    for e in range(NW):
        hbuf[e] = swiglu(acc[e])
    for p in range(NW // 2):
        start(p + NP)

    settle(gall, g_sem.at[0], gp_sem, None, (0, 2, 3, 1))
    here = (_dot(sall[...].reshape(4 * pair, 2 * n_exp), expand).reshape(4, pair, nk) == want)
    gs = gall[...].reshape(4 * pair, 2 * n_exp)
    hi = gs.astype(BF16)
    r1 = gs - hi.astype(F32)
    mid = r1.astype(BF16)
    lo = (r1 - mid.astype(F32)).astype(BF16)
    for k, p in enumerate((hi, mid, lo)):
        gt[:, pl.ds(k * pair, pair)] = jnp.where(here, _dot(p, expand).reshape(4, pair, nk), 0.0).astype(BF16)

    def up(u, _):
        for j in range(UP // 2):
            wait(u * (UP // 2) + j)
        for j in range(UP):
            w = ring[lax.rem(u * (UP // 2) + j // 2, NP), j % 2].reshape(n_k, KW, 2 * fl)
            two = pl.ds(u * UP + j // 2 * 2, 2)
            v = _dot(xg[0, two].reshape(2 * m, KW), w[0])
            for k in range(1, n_k):
                v = v + _dot(xg[k, two].reshape(2 * m, KW), w[k])
            hbuf[u * UP + j] = swiglu(own(v, j))
        for j in range(UP // 2):
            start(u * (UP // 2) + j + NP)
        return 0

    lax.fori_loop(NW // UP, n_el // UP, up, 0)

    wait_bytes(xall.at[pl.ds(0, n_k - 1)], x_sem.at[0])
    wait_bytes(xall.at[0, pl.ds(0, n_k // 2)], x_sem.at[0])
    for buf, sem in ((sall, s_sem), (gall, g_sem)):
        wait_bytes(buf.at[pl.ds(0, 3)], sem.at[0])
        wait_bytes(buf.at[0, pl.ds(0, t_loc)], sem.at[0])

    def y_copy(c):
        return remote(yacc.at[c, 1 - core], yrecv.at[c], y_sem.at[0], yr_sem.at[c], dev(0, True))

    halves = ((1, 2, pl.ds(0, CW // 2)), (2, 1, pl.ds(CW // 2, CW // 2)))

    def second(c):
        y_copy(c).wait_recv()
        yacc[c, core] += yrecv[c]

        @pl.when(c < NR)
        def _():
            for h, (r1, _, cols) in enumerate(halves):
                for k, r in enumerate((3, r1)):
                    remote(yacc.at[c, core, chip_of(r), :, cols], rmid.at[c, h, k], z_sem.at[0], zm_sem.at[c],
                           dev(r1, False)).start()

        @pl.when(c >= NR)
        def _():
            for r in (3, 1, 2):
                remote(yacc.at[c, core, chip_of(r)], rfin.at[c, r - 1], z_sem.at[0], zr_sem.at[c], dev(r, False)).start()

    def third(c):
        wait_bytes(rmid.at[c], zm_sem.at[c])
        for h, (_, r2, cols) in enumerate(halves):
            yacc[c, core, chip_of(r2), :, cols] += rmid[c, h, 0]
            yacc[c, core, chip, :, cols] += rmid[c, h, 1]
            remote(yacc.at[c, core, chip_of(r2), :, cols], rfin.at[c, 0, :, cols], z_sem.at[0], zr_sem.at[c],
                   dev(r2, False)).start()

    def products(c):
        for e in range(n_el):
            i, j = e // 8, e % 8
            w = ring[lax.rem(c + n_w13, NP), i % 2, j, :, (i // 2) * CW:(i // 2 + 1) * CW]
            y = own(_dot(hbuf[e // 2 * 2:e // 2 * 2 + 2].reshape(2 * m, fl), w), e)
            ybuf[e] = y.astype(BF16).reshape(4, 2 * cap, CW)

    def combine(c):
        for p in range(4):
            z = _dot(gt[p], ybuf[:, p].reshape(nk, CW))
            z = z[:pair] + z[pair:2 * pair] + z[2 * pair:]
            for k in range(2):
                yacc[c, k, p] = z[k * t_loc:(k + 1) * t_loc]

    def down(c, _):
        wait(n_w13 + c)
        products(c)
        combine(c)
        y_copy(c).start()

        @pl.when(c > 0)
        def _():
            second(c - 1)

        @pl.when(jnp.logical_and(c > 2, c - 3 < NR))
        def _():
            third(c - 3)

        return 0

    def o_copy(c):
        cols = pl.ds(pl.multiple_of(c * CW, CW), CW)
        return pltpu.make_async_copy(obuf.at[:, cols], o_ref.at[:, cols], o_sem.at[c])

    def total(c):
        cols = pl.ds(c * CW, CW)
        if c < NR:
            wait_bytes(rfin.at[c, 0], zr_sem.at[c])
            obuf[:, cols] = (yacc[c, core, chip] + rfin[c, 0]).astype(BF16)
        else:
            wait_bytes(rfin.at[c], zr_sem.at[c])
            obuf[:, cols] = (yacc[c, core, chip] + rfin[c, 0] + rfin[c, 1] + rfin[c, 2]).astype(BF16)
        o_copy(c).start()

    lax.fori_loop(0, n_chunk, down, 0)
    for c in range(2):
        total(c)
    second(n_chunk - 1)
    for c in range(2, n_chunk):
        total(c)
    for c in range(n_chunk):
        o_copy(c).wait()
    wait_bytes(yrecv, y_sem.at[0])
    wait_bytes(rfin, z_sem.at[0])


def solution(mesh):
    rows = P(("dp", "ep", "tp"), None)

    def local(x, idx, g, w1, w3, w2):
        t_loc, d = x.shape
        top = idx.shape[1]
        el, _, fl = w1.shape
        n_exp = 2 * el
        cap = CF * top * t_loc // n_exp
        nc = d // CW
        nk = el * 2 * cap
        dma, vm = pltpu.SemaphoreType.DMA, pltpu.VMEM
        any_ = pl.BlockSpec(memory_space=pl.ANY)
        y = pl.pallas_call(
            functools.partial(_kernel, el, cap),
            out_shape=jax.ShapeDtypeStruct((t_loc, d), BF16),
            in_specs=[any_] * 6,
            out_specs=any_,
            scratch_shapes=[
                vm((d // KW, 4, 2 * t_loc, KW), BF16),
                vm((top, t_loc), jnp.int32),
                vm((top, t_loc), F32),
                vm((4, 2 * t_loc, 2 * n_exp), BF16),
                vm((4, 2 * t_loc, 2 * n_exp), F32),
                vm((d // KW, el, 4, 2 * cap, KW), BF16),
                vm((NP, 2, d // fl, fl, 2 * fl), BF16),
                vm((NW, 8 * cap, 2 * fl), F32),
                vm((el, 8 * cap, fl), BF16),
                vm((4, 6 * t_loc, nk), BF16),
                vm((4, nk, 2 * t_loc), BF16),
                vm((el, 4, 2 * cap, CW), BF16),
                vm((nc, 2, 4, t_loc, CW), F32),
                vm((nc, 4, t_loc, CW), F32),
                vm((nc, 3, t_loc, CW), F32),
                dma((2 + d // KW,)), dma((NP,)),
                dma((1,)), dma((d // KW, 4)), dma((d // KW, 4)),
                dma((1,)), dma((4,)), dma((4,)),
                dma((1,)), dma((4,)), dma((4,)),
                dma((1,)), dma((nc,)), dma((1,)), dma((nc,)),
                vm((t_loc, d), BF16), dma((nc,)),
                vm((NR, 2, 2, t_loc, CW // 2), F32), dma((NR,)),
            ],
            compiler_params=pltpu.CompilerParams(collective_id=0, has_side_effects=True,
                                                 vmem_limit_bytes=67043328),
            name="moe",
        )(x, idx.T, g.T, w1.reshape(el, d // fl, fl, fl), w3.reshape(el, d // fl, fl, fl),
          w2.reshape(el // 8, 8, fl, d))
        return y

    return jax.shard_map(local, mesh=mesh,
                         in_specs=(rows, rows, rows, P("ep", None, "tp"), P("ep", None, "tp"), P("ep", "tp", None)),
                         out_specs=rows, check_vma=False)
```
